32 devices in a mesh: dp: 1 (over z), m3: 4 (over y), m2: 4 (over x), m1: 2 (over core).
Axes of the slice: x: 4, y: 4, z: 1, core: 2. Of those that a mesh axis runs over, the one named last changes fastest.
The devices are a block of a 4x4x8 slice.
Arguments:
- volume: bfloat16 [256, 64, 64, 64], P('dp', 'm1', 'm2', 'm3')
- fac_one: bfloat16 [64, 64], replicated
- fac_two: bfloat16 [64, 64], replicated
- fac_three: bfloat16 [64, 64], replicated
- diag_scale: float32 [64, 64, 64], P('m2', 'm1')
Outputs:
- output: bfloat16 [256, 64, 64, 64], P(('dp', 'm3'), 'm2', 'm1')
All inputs are finite; a program needn't handle non-finite values.
Results may differ from the reference program's by a relative error of at most 0.00844122.
Values are sent between devices in bfloat16 or wider.
A program may use at most 768 MiB of HBM per device.

```python
import jax
import jax.numpy as jnp
from jax import lax

GRID_ONE = 64
GRID_TWO = 64
GRID_THREE = 64
RHS_PART = 256


def orthonormal(rng_key, mat_order):
    gaussian = jax.random.normal(rng_key, (mat_order, mat_order), jnp.float32)
    ortho_mat = jnp.linalg.qr(gaussian)[0]
    return ortho_mat.astype(jnp.bfloat16)


def setup_inputs(seed: int = 0, part: int = 0) -> dict:
    base_key = jax.random.key(seed)
    key_list = jax.random.split(base_key, 5)
    vol_key = jax.random.fold_in(key_list[0], part)
    volume = jax.random.normal(vol_key, (RHS_PART, GRID_ONE, GRID_TWO, GRID_THREE), jnp.float32).astype(jnp.bfloat16)
    fac_one = orthonormal(key_list[1], GRID_ONE)
    fac_two = orthonormal(key_list[2], GRID_TWO)
    fac_three = orthonormal(key_list[3], GRID_THREE)
    log_diag = jax.random.uniform(key_list[4], (GRID_THREE, GRID_TWO, GRID_ONE), jnp.float32, -1.15, 1.15)
    diag_scale = jnp.exp(log_diag)
    return {"volume": volume, "fac_one": fac_one, "fac_two": fac_two, "fac_three": fac_three, "diag_scale": diag_scale}


def reference(volume, fac_one, fac_two, fac_three, diag_scale):
    one_wide = fac_one.astype(jnp.float32)
    two_wide = fac_two.astype(jnp.float32)
    three_wide = fac_three.astype(jnp.float32)

    def per_rhs(vol_one):
        prod_three = jnp.einsum("abl,kl->abk", vol_one.astype(jnp.float32), three_wide).astype(jnp.bfloat16)
        prod_two = jnp.einsum("abk,jb->akj", prod_three.astype(jnp.float32), two_wide).astype(jnp.bfloat16)
        prod_one = jnp.einsum("akj,ia->kji", prod_two.astype(jnp.float32), one_wide).astype(jnp.bfloat16)
        return (diag_scale * prod_one.astype(jnp.float32)).astype(jnp.bfloat16)

    return lax.map(per_rhs, volume)
```

```python
import functools

import jax
import jax.numpy as jnp
from jax import lax
from jax.experimental import pallas as pl
from jax.experimental.pallas import tpu as pltpu
from jax.sharding import PartitionSpec as P

MESH = pl.DeviceIdType.MESH
BF16, F32 = jnp.bfloat16, jnp.float32
SG = 8
PIECES = 2
X_PARTS = 4


def dot(lhs, rhs, contract=((1,), (0,))):
    return lax.dot_general(lhs, rhs, (contract, ((), ())), preferred_element_type=F32)


def iota(shape, dim):
    return lax.broadcasted_iota(jnp.int32, shape, dim)


def onehot(cond):
    return jnp.where(cond, 1.0, 0.0).astype(BF16)


def kernel(dims, x_hbm, a1_hbm, a2_hbm, a3_hbm, d_hbm, out, xbuf, tbuf, r1, u3, r2, v2, r3, w1, w2, w3, ident, a1, a2, a3, dbuf,
           in_sem, fac_sem, y_send, y_recv, x_send, x_recv, c_send, c_recv):
    n3, n2, n1, na, nb, nl, ns, nk, nj, ni = dims
    me3, me2, me1 = lax.axis_index("m3"), lax.axis_index("m2"), lax.axis_index("m1")
    groups = ns // n3 // SG
    rows = na * SG
    pairs = na // 2
    ppp = pairs // PIECES
    prow = rows // PIECES
    kb, jb = nk // n2, nj // n1
    bl, bk, kj = nb * nl, nb * kb, kb * jb

    loads = []
    apart = na // X_PARTS
    for h in range(X_PARTS):
        part = pl.ds(h * apart, apart)
        loads.append(pltpu.make_async_copy(x_hbm.at[part], xbuf.at[part], in_sem.at[h]))
        loads[-1].start()
    facs = [pltpu.make_async_copy(s, t, fac_sem.at[i]) for i, (s, t) in enumerate(((a3_hbm, a3), (a2_hbm, a2), (a1_hbm, a1), (d_hbm, dbuf)))]
    for f in facs:
        f.start()

    barrier = pltpu.get_barrier_semaphore()
    peers = 0
    for axis, me, n in (("m3", me3, n3), ("m2", me2, n2), ("m1", me1, n1)):
        for d in range(1, n):
            pl.semaphore_signal(barrier, inc=1, device_id={axis: lax.rem(me + d, n)}, device_id_type=MESH)
            peers += 1

    sd = ns // n3
    r, c = iota((ns, ns), 0), iota((ns, ns), 1)
    want = lax.rem(r // sd + me3, n3) * sd + lax.rem(r, sd)
    ident[...] = onehot(c == want)

    def y_copy(d, g, p):
        at = pl.ds(p * ppp, ppp)
        return pltpu.make_async_remote_copy(
            src_ref=tbuf.at[d, g, at], dst_ref=r1.at[d - 1, g, at], send_sem=y_send.at[d - 1, g * PIECES + p],
            recv_sem=y_recv.at[d - 1, g * PIECES + p], device_id={"m3": lax.rem(me3 + d, n3)}, device_id_type=MESH)

    def x_copy(d, g, p):
        at = pl.ds(p * prow, prow)
        return pltpu.make_async_remote_copy(
            src_ref=u3.at[d, g, at], dst_ref=r2.at[d - 1, g, at], send_sem=x_send.at[d - 1, g * PIECES + p],
            recv_sem=x_recv.at[d - 1, g * PIECES + p], device_id={"m2": lax.rem(me2 + d, n2)}, device_id_type=MESH)

    def c_copy(g):
        return pltpu.make_async_remote_copy(
            src_ref=v2.at[1, g], dst_ref=r3.at[g], send_sem=c_send.at[g], recv_sem=c_recv.at[g],
            device_id={"m1": lax.rem(me1 + 1, n1)}, device_id_type=MESH)

    eye = ident[...]
    per = pairs // X_PARTS
    for h in range(X_PARTS):
        loads[h].wait()

        def turn(i, carry):
            ap = h * per + i
            f0 = dot(eye, xbuf[2 * ap].reshape(bl, ns), ((1,), (1,)))
            f1 = dot(eye, xbuf[2 * ap + 1].reshape(bl, ns), ((1,), (1,)))
            both = jnp.stack([f0.reshape(ns // SG, SG, bl), f1.reshape(ns // SG, SG, bl)], axis=1)
            tbuf[:, :, ap] = both.reshape(n3, groups, 2 * SG, bl).astype(BF16)
            return carry

        lax.fori_loop(0, per, turn, 0)
        if h == 0:
            pl.semaphore_wait(barrier, peers)
        if (h + 1) % (X_PARTS // PIECES) == 0:
            for d in range(1, n3):
                y_copy(d, 0, h // (X_PARTS // PIECES)).start()

    def send_rest(g, carry):
        for p in range(PIECES):
            for d in range(1, n3):
                y_copy(d, g, p).start()
        return carry

    lax.fori_loop(1, groups, send_rest, 0)

    for f in facs:
        f.wait()
    c = iota((nk, n2 * bk), 1)
    pick = onehot(iota((nk, n2 * bk), 0) == lax.rem(c // bk + me2, n2) * kb + lax.rem(c, kb))
    cols3 = dot(a3[...], pick, ((0,), (0,))).astype(BF16)
    r, c = iota((bl, n2 * bk), 0), iota((bl, n2 * bk), 1)
    same_b = r // nl == lax.rem(c // kb, nb)
    for d in range(n3):
        r = iota((bl, n3 * nl), 0)
        sel = onehot(iota((bl, n3 * nl), 1) == lax.rem(me3 - d + n3, n3) * nl + lax.rem(r, nl))
        w1[d * bl : (d + 1) * bl, :] = jnp.where(same_b, dot(sel, cols3), 0.0).astype(BF16)

    c = iota((n2 * nb, n2 * bk), 1)
    pick = onehot(iota((n2 * nb, n2 * bk), 0) == lax.rem(me2 - c // bk + n2, n2) * nb + lax.rem(c // kb, nb))
    cols2 = dot(a2[...], pick).astype(BF16)
    r, c = iota((kj, n2 * bk), 0), iota((kj, n2 * bk), 1)
    same_k = r // jb == lax.rem(c, kb)
    for e in range(n1):
        r = iota((kj, nj), 0)
        sel = onehot(iota((kj, nj), 1) == lax.rem(me1 + e, n1) * jb + lax.rem(r, jb))
        w2[e * kj : (e + 1) * kj, :] = jnp.where(same_k, dot(sel, cols2), 0.0).astype(BF16)

    wide = 2 * ni
    c = iota((ni, SG * wide), 1)
    pick = onehot(iota((ni, SG * wide), 0) == lax.rem(c, wide))
    cols1 = dot(a1[...], pick, ((0,), (0,))).astype(BF16)
    r, c = iota((rows, SG * wide), 0), iota((rows, SG * wide), 1)
    same_s = lax.rem(r, SG) == c // wide
    for e in range(n1):
        r = iota((rows, n1 * na), 0)
        sel = onehot(iota((rows, n1 * na), 1) == lax.rem(me1 + e, n1) * na + r // SG)
        w3[e * rows : (e + 1) * rows, :] = jnp.where(same_s, dot(sel, cols1), 0.0).astype(BF16)

    def stage1(g, p):
        for d in range(1, n3):
            y_copy(d, g, p).wait_recv()
        at = pl.ds(p * ppp, ppp)
        lhs = [tbuf[0, g, at].reshape(prow, bl)] + [r1[d, g, at].reshape(prow, bl) for d in range(n3 - 1)]
        lhs = jnp.concatenate(lhs, axis=1)
        for d in (*range(1, n2), 0):
            u3[d, g, pl.ds(p * prow, prow)] = dot(lhs, w1[:, d * bk : (d + 1) * bk]).astype(BF16)
            if d:
                x_copy(d, g, p).start()

    def stage2(g):
        for p in range(PIECES):
            for d in range(1, n2):
                x_copy(d, g, p).wait_recv()
        rhs = jnp.concatenate([u3[0, g]] + [r2[d, g] for d in range(n2 - 1)], axis=1)
        for e in (1, 0):
            v2[e, g] = dot(w2[e * kj : (e + 1) * kj, :], rhs, ((1,), (1,))).astype(BF16)
            if e:
                c_copy(g).start()

    def stage3(g):
        c_copy(g).wait_recv()
        lhs = jnp.concatenate([v2[0, g], r3[g]], axis=1)
        scale = dbuf[...].reshape(kj, ni)
        for q in range(SG // 2):
            prod = dot(lhs, w3[:, q * 2 * wide : (q + 1) * 2 * wide]).astype(BF16)
            for i in range(2):
                one = prod[:, i * wide : i * wide + ni].astype(F32)
                out[g * SG + 2 * q + i] = (scale * one).astype(BF16).reshape(kb, jb, ni)

    def step(t, carry):
        @pl.when(t < groups)
        def _():
            for p in range(PIECES):
                stage1(t, p)

        @pl.when(jnp.logical_and(t >= 2, t < groups + 2))
        def _():
            stage2(t - 2)

        @pl.when(t >= 3)
        def _():
            stage3(t - 3)

        return carry

    lax.fori_loop(0, groups + 3, step, 0)

    def drain(g, carry):
        for p in range(PIECES):
            for d in range(1, n3):
                y_copy(d, g, p).wait_send()
            for d in range(1, n2):
                x_copy(d, g, p).wait_send()
        c_copy(g).wait_send()
        return carry

    lax.fori_loop(0, groups, drain, 0)


def solution(mesh):
    n3, n2, n1 = mesh.shape["m3"], mesh.shape["m2"], mesh.shape["m1"]

    def local_step(vol_blk, fac_one, fac_two, fac_three, diag_blk):
        ns, na, nb, nl = vol_blk.shape
        nk, nj, ni = fac_three.shape[0], fac_two.shape[0], fac_one.shape[0]
        kb, jb = nk // n2, nj // n1
        groups, rows = ns // n3 // SG, na * SG
        bl, bk, kj = nb * nl, nb * kb, kb * jb
        dims = (n3, n2, n1, na, nb, nl, ns, nk, nj, ni)
        dma = pltpu.SemaphoreType.DMA
        any_space = pl.BlockSpec(memory_space=pl.ANY)
        scratch = [
            pltpu.VMEM((na, nb, nl, ns), BF16),
            pltpu.VMEM((n3, groups, na // 2, 2 * SG, bl), BF16),
            pltpu.VMEM((n3 - 1, groups, na // 2, 2 * SG, bl), BF16),
            pltpu.VMEM((n2, groups, rows, bk), BF16),
            pltpu.VMEM((n2 - 1, groups, rows, bk), BF16),
            pltpu.VMEM((n1, groups, kj, rows), BF16),
            pltpu.VMEM((groups, kj, rows), BF16),
            pltpu.VMEM((n3 * bl, n2 * bk), BF16),
            pltpu.VMEM((n1 * kj, n2 * bk), BF16),
            pltpu.VMEM((n1 * rows, SG * 2 * ni), BF16),
            pltpu.VMEM((ns, ns), BF16),
            pltpu.VMEM(fac_one.shape, BF16),
            pltpu.VMEM(fac_two.shape, BF16),
            pltpu.VMEM(fac_three.shape, BF16),
            pltpu.VMEM(diag_blk.shape, F32),
            dma((X_PARTS,)), dma((4,)),
            dma((n3 - 1, groups * PIECES)), dma((n3 - 1, groups * PIECES)),
            dma((n2 - 1, groups * PIECES)), dma((n2 - 1, groups * PIECES)),
            dma((groups,)), dma((groups,)),
        ]
        call = pl.pallas_call(
            functools.partial(kernel, dims),
            out_shape=pltpu.VMEM((ns // n3, kb, jb, ni), BF16),
            in_specs=[any_space] * 5,
            out_specs=pl.BlockSpec(memory_space=pltpu.VMEM),
            scratch_shapes=scratch,
            compiler_params=pltpu.CompilerParams(collective_id=0, has_side_effects=True, vmem_limit_bytes=50 * 1024 * 1024),
        )
        return call(jnp.transpose(vol_blk, (1, 2, 3, 0)), fac_one, fac_two, fac_three, diag_blk)

    return jax.shard_map(local_step, mesh=mesh, in_specs=(P("dp", "m1", "m2", "m3"), P(), P(), P(), P("m2", "m1", None)), out_specs=P(("dp", "m3"), "m2", "m1", None), check_vma=False)
```

```python
import functools

import jax
import jax.numpy as jnp
from jax import lax
from jax.experimental import pallas as pl
from jax.experimental.pallas import tpu as pltpu
from jax.sharding import PartitionSpec as P

MESH = pl.DeviceIdType.MESH
BF16, F32 = jnp.bfloat16, jnp.float32
SG = 8
PIECES = 4
AHEAD = 3
LANES = 128


def far_first(n):
    return sorted(range(1, n), key=lambda d: -min(d, n - d))


def dot(lhs, rhs, contract=((1,), (0,))):
    return lax.dot_general(lhs, rhs, (contract, ((), ())), preferred_element_type=F32)


def iota(shape, dim):
    return lax.broadcasted_iota(jnp.int32, shape, dim)


def onehot(cond):
    return jnp.where(cond, 1.0, 0.0).astype(BF16)


def kernel(dims, x_hbm, a1_hbm, a2_hbm, a3_hbm, d_hbm, out, xbuf, tbuf, r1, u3, r2, v2, r3, w1, w2, w3, ident, a1, a2, a3, dbuf,
           in_sem, fac_sem, y_send, y_recv, x_send, x_recv, c_send, c_recv):
    n3, n2, n1, na, nb, nl, ns, nk, nj, ni = dims
    me3, me2, me1 = lax.axis_index("m3"), lax.axis_index("m2"), lax.axis_index("m1")
    groups = ns // n3 // SG
    rows = na * SG
    pairs = na // 2
    ppp = pairs // PIECES
    prow = rows // PIECES
    kb, jb = nk // n2, nj // n1
    bl, bk, kj = nb * nl, nb * kb, kb * jb
    bt, kt = bl // LANES, bk // LANES
    bs, ks = nb // bt, kb // kt
    half = ks * jb

    facs = [pltpu.make_async_copy(s, t, fac_sem.at[i]) for i, (s, t) in enumerate(((a3_hbm, a3), (a2_hbm, a2), (a1_hbm, a1), (d_hbm, dbuf)))]
    facs[0].start()
    loads = []
    apart = na // PIECES
    for h in range(PIECES):
        part = pl.ds(h * apart, apart)
        loads.append(pltpu.make_async_copy(x_hbm.at[part], xbuf.at[part], in_sem.at[h]))
        loads[-1].start()
    for f in facs[1:]:
        f.start()

    barrier = pltpu.get_barrier_semaphore()
    peers = 0
    for axis, me, n in (("m3", me3, n3), ("m2", me2, n2), ("m1", me1, n1)):
        for d in range(1, n):
            pl.semaphore_signal(barrier, inc=1, device_id={axis: lax.rem(me + d, n)}, device_id_type=MESH)
            peers += 1

    def y_copy(src, dst, sem, d=1):
        return pltpu.make_async_remote_copy(src_ref=src, dst_ref=dst, send_sem=y_send, recv_sem=y_recv.at[sem],
                                            device_id={"m3": lax.rem(me3 + d, n3)}, device_id_type=MESH)

    def x_copy(src, dst, sem, d=1):
        return pltpu.make_async_remote_copy(src_ref=src, dst_ref=dst, send_sem=x_send, recv_sem=x_recv.at[sem],
                                            device_id={"m2": lax.rem(me2 + d, n2)}, device_id_type=MESH)

    def c_copy(src, dst, sem):
        return pltpu.make_async_remote_copy(src_ref=src, dst_ref=dst, send_sem=c_send, recv_sem=c_recv.at[sem],
                                            device_id={"m1": lax.rem(me1 + 1, n1)}, device_id_type=MESH)

    def send_piece(g, p):
        at = pl.ds(p * ppp, ppp)
        for d in far_first(n3):
            y_copy(tbuf.at[d, g, at], r1.at[d - 1, g, at], g * PIECES + p, d).start()

    def send_group(g):
        for p in range(PIECES):
            send_piece(g, p)

    sd = ns // n3
    r, c = iota((ns, ns), 0), iota((ns, ns), 1)
    ident[...] = onehot(c == lax.rem(r // sd + me3, n3) * sd + lax.rem(r, sd))

    c = iota((nk, n2 * LANES), 1)
    k_of = lax.rem(c, LANES) // (LANES // kt) * ks + lax.rem(c, ks)
    pick = onehot(iota((nk, n2 * LANES), 0) == lax.rem(c // LANES + me2, n2) * kb + k_of)
    r, c = iota((LANES, n2 * LANES), 0), iota((LANES, n2 * LANES), 1)
    same_b = r // nl == lax.rem(c // ks, bs)
    facs[0].wait()
    cols3 = dot(a3[...], pick, ((0,), (0,))).astype(BF16)
    for d in range(n3):
        r = iota((LANES, n3 * nl), 0)
        sel = onehot(iota((LANES, n3 * nl), 1) == lax.rem(me3 - d + n3, n3) * nl + lax.rem(r, nl))
        w1[d * LANES : (d + 1) * LANES, :] = jnp.where(same_b, dot(sel, cols3), 0.0).astype(BF16)

    def build_rest():
        for f in facs[1:]:
            f.wait()
        c = iota((n2 * nb, n2 * LANES), 1)
        pick = onehot(iota((n2 * nb, n2 * LANES), 0) == lax.rem(me2 - c // LANES + n2, n2) * nb + lax.rem(c, LANES) // ks)
        cols2 = dot(a2[...], pick).astype(BF16)
        r, c = iota((half, n2 * LANES), 0), iota((half, n2 * LANES), 1)
        same_k = r // jb == lax.rem(c, ks)
        for e in range(n1):
            r = iota((half, nj), 0)
            sel = onehot(iota((half, nj), 1) == lax.rem(me1 + e, n1) * jb + lax.rem(r, jb))
            w2[e * half : (e + 1) * half, :] = jnp.where(same_k, dot(sel, cols2), 0.0).astype(BF16)

        c = iota((ni, SG * wide), 1)
        pick = onehot(iota((ni, SG * wide), 0) == lax.rem(c, wide))
        cols1 = dot(a1[...], pick, ((0,), (0,))).astype(BF16)
        r, c = iota((rows, SG * wide), 0), iota((rows, SG * wide), 1)
        same_s = lax.rem(r, SG) == c // wide
        for e in range(n1):
            r = iota((rows, n1 * na), 0)
            sel = onehot(iota((rows, n1 * na), 1) == lax.rem(me1 + e, n1) * na + r // SG)
            w3[e * rows : (e + 1) * rows, :] = jnp.where(same_s, dot(sel, cols1), 0.0).astype(BF16)

    wide = 2 * ni
    eye = ident[...]
    for h in range(PIECES):
        loads[h].wait()
        for ap in range(h * ppp, (h + 1) * ppp):
            two = [dot(eye, xbuf[2 * ap + i].reshape(bl, ns), ((1,), (1,))).reshape(ns // SG, SG, bl) for i in range(2)]
            tbuf[:, :, ap] = jnp.stack(two, axis=1).reshape(n3, groups, 2 * SG, bl).astype(BF16)
        if h == 0:
            pl.semaphore_wait(barrier, peers)
        send_piece(0, h)
    for g in range(1, AHEAD):
        send_group(g)

    def stage1(g, p):
        at = pl.ds(p * ppp, ppp)
        y_copy(tbuf.at[pl.ds(1, n3 - 1), g, at], r1.at[:, g, at], g * PIECES + p).wait_recv()
        got = [tbuf[0, g, at].reshape(prow, bl)] + [r1[d, g, at].reshape(prow, bl) for d in range(n3 - 1)]
        lhs = [jnp.concatenate([v[:, t * LANES : (t + 1) * LANES] for v in got], axis=1) for t in range(bt)]
        prod = dot(jnp.concatenate(lhs, axis=0), w1[...])
        width = LANES // bt
        slot = iota((prow, LANES), 1) // width
        at = pl.ds(p * prow, prow)
        for d in (*far_first(n2), 0):
            by_b = [prod[t * prow : (t + 1) * prow, d * LANES : (d + 1) * LANES] for t in range(bt)]
            for u in range(kt):
                tile = by_b[u]
                for t in range(bt):
                    if t != u:
                        tile = jnp.where(slot == t, pltpu.roll(by_b[t], (t - u) * width % LANES, 1), tile)
                u3[d, g, at, u * LANES : (u + 1) * LANES] = tile.astype(BF16)
            if d:
                x_copy(u3.at[d, g, at], r2.at[d - 1, g, at], g, d).start()

    def stage2(g):
        x_copy(u3.at[pl.ds(1, n2 - 1), g], r2.at[:, g], g).wait_recv()
        got = [u3.at[0, g]] + [r2.at[d, g] for d in range(n2 - 1)]
        for u in range(kt):
            rhs = jnp.concatenate([v[:, u * LANES : (u + 1) * LANES] for v in got], axis=1)
            prod = dot(w2[...], rhs, ((1,), (1,))).astype(BF16)
            at = pl.ds(u * half, half)
            for e in range(n1 - 1, -1, -1):
                v2[e, g, at] = prod[e * half : (e + 1) * half, :]
            c_copy(v2.at[1, g, at], r3.at[g, at], g).start()

    def stage3(g):
        c_copy(v2.at[1, g], r3.at[g], g).wait_recv()
        lhs = jnp.concatenate([v2[0, g], r3[g]], axis=1)
        scale = dbuf[...].reshape(kj, ni)
        for q in range(SG // 2):
            prod = dot(lhs, w3[:, q * 2 * wide : (q + 1) * 2 * wide]).astype(BF16)
            for i in range(2):
                one = prod[:, i * wide : i * wide + ni].astype(F32)
                out[g * SG + 2 * q + i] = (scale * one).astype(BF16).reshape(kb, jb, ni)

    def step(g, carry):
        for p in range(PIECES):
            stage1(g, p)
            if p == PIECES - 2:
                pl.when(g >= 2)(lambda: stage3(g - 2))
        pl.when(g + AHEAD < groups)(lambda: send_group(g + AHEAD))
        pl.when(g == 0)(build_rest)
        pl.when(g >= 1)(lambda: stage2(g - 1))
        return carry

    lax.fori_loop(0, groups, step, 0)
    stage3(groups - 2)
    stage2(groups - 1)
    stage3(groups - 1)

    y_copy(tbuf.at[pl.ds(1, n3 - 1)], r1, 0).wait_send()
    x_copy(u3.at[pl.ds(1, n2 - 1)], r2, 0).wait_send()
    c_copy(v2.at[1], r3, 0).wait_send()


def solution(mesh):
    n3, n2, n1 = mesh.shape["m3"], mesh.shape["m2"], mesh.shape["m1"]

    def local_step(vol_blk, fac_one, fac_two, fac_three, diag_blk):
        ns, na, nb, nl = vol_blk.shape
        nk, nj, ni = fac_three.shape[0], fac_two.shape[0], fac_one.shape[0]
        kb, jb = nk // n2, nj // n1
        groups, rows = ns // n3 // SG, na * SG
        bl, bk, kj = nb * nl, nb * kb, kb * jb
        dims = (n3, n2, n1, na, nb, nl, ns, nk, nj, ni)
        dma = pltpu.SemaphoreType.DMA
        any_space = pl.BlockSpec(memory_space=pl.ANY)
        scratch = [
            pltpu.VMEM((na, nb, nl, ns), BF16),
            pltpu.VMEM((n3, groups, na // 2, 2 * SG, bl), BF16),
            pltpu.VMEM((n3 - 1, groups, na // 2, 2 * SG, bl), BF16),
            pltpu.VMEM((n2, groups, rows, bk), BF16),
            pltpu.VMEM((n2 - 1, groups, rows, bk), BF16),
            pltpu.VMEM((n1, groups, kj, rows), BF16),
            pltpu.VMEM((groups, kj, rows), BF16),
            pltpu.VMEM((n3 * LANES, n2 * LANES), BF16),
            pltpu.VMEM((n1 * kj * LANES // bk, n2 * LANES), BF16),
            pltpu.VMEM((n1 * rows, SG * 2 * ni), BF16),
            pltpu.VMEM((ns, ns), BF16),
            pltpu.VMEM(fac_one.shape, BF16),
            pltpu.VMEM(fac_two.shape, BF16),
            pltpu.VMEM(fac_three.shape, BF16),
            pltpu.VMEM(diag_blk.shape, F32),
            dma((PIECES,)), dma((4,)), dma, dma((groups * PIECES,)), dma, dma((groups,)), dma, dma((groups,)),
        ]
        call = pl.pallas_call(
            functools.partial(kernel, dims),
            out_shape=pltpu.VMEM((ns // n3, kb, jb, ni), BF16),
            in_specs=[any_space] * 5,
            out_specs=pl.BlockSpec(memory_space=pltpu.VMEM),
            scratch_shapes=scratch,
            compiler_params=pltpu.CompilerParams(collective_id=0, has_side_effects=True, vmem_limit_bytes=50 * 1024 * 1024),
        )
        return call(jnp.transpose(vol_blk, (1, 2, 3, 0)), fac_one, fac_two, fac_three, diag_blk)

    return jax.shard_map(local_step, mesh=mesh, in_specs=(P("dp", "m1", "m2", "m3"), P(), P(), P(), P("m2", "m1", None)), out_specs=P(("dp", "m3"), "m2", "m1", None), check_vma=False)
```

```python
import functools

import jax
import jax.numpy as jnp
from jax import lax
from jax.experimental import pallas as pl
from jax.experimental.pallas import tpu as pltpu
from jax.sharding import PartitionSpec as P

MESH = pl.DeviceIdType.MESH
BF16, F32 = jnp.bfloat16, jnp.float32
SG = 8
PIECES = 4
FIRST = (2, 2, 4, 4, 4)
COPIES = 7
AHEAD = 3
LANES = 128


def far_first(n):
    return sorted(range(1, n), key=lambda d: -min(d, n - d))


def dot(lhs, rhs, contract=((1,), (0,))):
    return lax.dot_general(lhs, rhs, (contract, ((), ())), preferred_element_type=F32)


def iota(shape, dim):
    return lax.broadcasted_iota(jnp.int32, shape, dim)


def onehot(cond):
    return jnp.where(cond, 1.0, 0.0).astype(BF16)


def third(lhs, w3, d_ref, out, base, shape):
    ni = shape[-1]
    wide = w3.shape[1] // SG
    scale = d_ref[...].reshape(-1, ni)
    for q in range(SG // 2):
        prod = dot(lhs, w3[:, q * 2 * wide : (q + 1) * 2 * wide]).astype(BF16)
        for i in range(2):
            one = prod[:, i * wide : i * wide + ni].astype(F32)
            out[base + 2 * q + i] = (scale * one).astype(BF16).reshape(shape)


def finish(done, last, w3, d_ref, out, tail, sem):
    size = done.shape[0]
    chunk = size // COPIES
    copies = [pltpu.make_async_copy(done.at[pl.ds(i * chunk, chunk)], out.at[pl.ds(i * chunk, chunk)], sem.at[i]) for i in range(COPIES)]
    for c in copies:
        c.start()
    third(last[...], w3, d_ref, tail, 0, tail.shape[1:])
    copies.append(pltpu.make_async_copy(tail, out.at[pl.ds(size, SG)], sem.at[COPIES]))
    copies[-1].start()
    for c in copies:
        c.wait()


def kernel(dims, x_hbm, a1_hbm, a2_hbm, a3_hbm, d_hbm, out, last, w3, dbuf, xbuf, tbuf, r1, u3, r2, v2, r3, w1, w2, ident, a1, a2, a3,
           in_sem, fac_sem, y_send, y_recv, x_send, x_recv, c_send, c_recv):
    n3, n2, n1, na, nb, nl, ns, nk, nj, ni = dims
    me3, me2, me1 = lax.axis_index("m3"), lax.axis_index("m2"), lax.axis_index("m1")
    groups = ns // n3 // SG
    rows = na * SG
    pairs = na // 2
    ppp = pairs // PIECES
    prow = rows // PIECES
    kb, jb = nk // n2, nj // n1
    bl, bk, kj = nb * nl, nb * kb, kb * jb
    bt, kt = bl // LANES, bk // LANES
    bs, ks = nb // bt, kb // kt
    half = ks * jb

    loads, cuts = [], [0]
    for n in FIRST:
        part = pl.ds(2 * cuts[-1], 2 * n)
        loads.append(pltpu.make_async_copy(x_hbm.at[part], xbuf.at[part], in_sem.at[len(loads)]))
        cuts.append(cuts[-1] + n)
    facs = [pltpu.make_async_copy(s, t, fac_sem.at[i]) for i, (s, t) in enumerate(((a3_hbm, a3), (a2_hbm, a2), (a1_hbm, a1), (d_hbm, dbuf)))]
    loads[0].start()

    barrier = pltpu.get_barrier_semaphore()
    peers = 0
    for axis, me, n in (("m3", me3, n3), ("m2", me2, n2), ("m1", me1, n1)):
        for d in range(1, n):
            pl.semaphore_signal(barrier, inc=1, device_id={axis: lax.rem(me + d, n)}, device_id_type=MESH)
            peers += 1
    for f in loads[1:] + facs:
        f.start()

    def y_copy(src, dst, sem, d=1):
        return pltpu.make_async_remote_copy(src_ref=src, dst_ref=dst, send_sem=y_send, recv_sem=y_recv.at[sem],
                                            device_id={"m3": lax.rem(me3 + d, n3)}, device_id_type=MESH)

    def x_copy(src, dst, sem, d=1):
        return pltpu.make_async_remote_copy(src_ref=src, dst_ref=dst, send_sem=x_send, recv_sem=x_recv.at[sem],
                                            device_id={"m2": lax.rem(me2 + d, n2)}, device_id_type=MESH)

    def c_copy(src, dst, sem):
        return pltpu.make_async_remote_copy(src_ref=src, dst_ref=dst, send_sem=c_send, recv_sem=c_recv.at[sem],
                                            device_id={"m1": lax.rem(me1 + 1, n1)}, device_id_type=MESH)

    def send_pairs(g, lo, n):
        at = pl.ds(lo, n)
        for d in far_first(n3):
            y_copy(tbuf.at[d, g, at], r1.at[d - 1, g, at], g * PIECES + lo // ppp, d).start()

    def send_group(g):
        for p in range(PIECES):
            send_pairs(g, p * ppp, ppp)

    sd = ns // n3
    r, c = iota((ns, ns), 0), iota((ns, ns), 1)
    ident[...] = onehot(c == lax.rem(r // sd + me3, n3) * sd + lax.rem(r, sd))

    def build_rest():
        for f in facs[1:]:
            f.wait()
        c = iota((n2 * nb, n2 * LANES), 1)
        pick = onehot(iota((n2 * nb, n2 * LANES), 0) == lax.rem(me2 - c // LANES + n2, n2) * nb + lax.rem(c, LANES) // ks)
        cols2 = dot(a2[...], pick).astype(BF16)
        r, c = iota((half, n2 * LANES), 0), iota((half, n2 * LANES), 1)
        same_k = r // jb == lax.rem(c, ks)
        for e in range(n1):
            r = iota((half, nj), 0)
            sel = onehot(iota((half, nj), 1) == lax.rem(me1 + e, n1) * jb + lax.rem(r, jb))
            w2[e * half : (e + 1) * half, :] = jnp.where(same_k, dot(sel, cols2), 0.0).astype(BF16)

        c = iota((ni, SG * wide), 1)
        pick = onehot(iota((ni, SG * wide), 0) == lax.rem(c, wide))
        cols1 = dot(a1[...], pick, ((0,), (0,))).astype(BF16)
        r, c = iota((rows, SG * wide), 0), iota((rows, SG * wide), 1)
        same_s = lax.rem(r, SG) == c // wide
        for e in range(n1):
            r = iota((rows, n1 * na), 0)
            sel = onehot(iota((rows, n1 * na), 1) == lax.rem(me1 + e, n1) * na + r // SG)
            w3[e * rows : (e + 1) * rows, :] = jnp.where(same_s, dot(sel, cols1), 0.0).astype(BF16)

    wide = 2 * ni
    eye = ident[...]
    for h, n in enumerate(FIRST):
        loads[h].wait()
        for ap in range(cuts[h], cuts[h + 1]):
            two = [dot(eye, xbuf[2 * ap + i].reshape(bl, ns), ((1,), (1,))).reshape(ns // SG, SG, bl) for i in range(2)]
            tbuf[:, :, ap] = jnp.stack(two, axis=1).reshape(n3, groups, 2 * SG, bl).astype(BF16)
        if h == 0:
            pl.semaphore_wait(barrier, peers)
        send_pairs(0, cuts[h], n)

    c = iota((nk, n2 * LANES), 1)
    k_of = lax.rem(c, LANES) // (LANES // kt) * ks + lax.rem(c, ks)
    pick = onehot(iota((nk, n2 * LANES), 0) == lax.rem(c // LANES + me2, n2) * kb + k_of)
    r, c = iota((LANES, n2 * LANES), 0), iota((LANES, n2 * LANES), 1)
    same_b = r // nl == lax.rem(c // ks, bs)
    facs[0].wait()
    cols3 = dot(a3[...], pick, ((0,), (0,))).astype(BF16)
    for d in range(n3):
        r = iota((LANES, n3 * nl), 0)
        sel = onehot(iota((LANES, n3 * nl), 1) == lax.rem(me3 - d + n3, n3) * nl + lax.rem(r, nl))
        w1[d * LANES : (d + 1) * LANES, :] = jnp.where(same_b, dot(sel, cols3), 0.0).astype(BF16)

    for g in range(1, AHEAD):
        send_group(g)

    def stage1(g, p):
        at = pl.ds(p * ppp, ppp)
        y_copy(tbuf.at[pl.ds(1, n3 - 1), g, at], r1.at[:, g, at], g * PIECES + p).wait_recv()
        got = [tbuf[0, g, at].reshape(prow, bl)] + [r1[d, g, at].reshape(prow, bl) for d in range(n3 - 1)]
        lhs = [jnp.concatenate([v[:, t * LANES : (t + 1) * LANES] for v in got], axis=1) for t in range(bt)]
        prod = dot(jnp.concatenate(lhs, axis=0), w1[...])
        width = LANES // bt
        slot = iota((prow, LANES), 1) // width
        at = pl.ds(p * prow, prow)
        for d in (*far_first(n2), 0):
            by_b = [prod[t * prow : (t + 1) * prow, d * LANES : (d + 1) * LANES] for t in range(bt)]
            for u in range(kt):
                tile = by_b[u]
                for t in range(bt):
                    if t != u:
                        tile = jnp.where(slot == t, pltpu.roll(by_b[t], (t - u) * width % LANES, 1), tile)
                u3[d, g, at, u * LANES : (u + 1) * LANES] = tile.astype(BF16)
            if d:
                x_copy(u3.at[d, g, at], r2.at[d - 1, g, at], g, d).start()

    def stage2(g, final=False):
        x_copy(u3.at[pl.ds(1, n2 - 1), g], r2.at[:, g], g).wait_recv()
        got = [u3.at[0, g]] + [r2.at[d, g] for d in range(n2 - 1)]
        for es in ((1,), (0,)) if final else (tuple(range(n1)),):
            for u in range(kt):
                rhs = jnp.concatenate([v[:, u * LANES : (u + 1) * LANES] for v in got], axis=1)
                prod = dot(w2[es[0] * half : (es[-1] + 1) * half, :], rhs, ((1,), (1,))).astype(BF16)
                at = pl.ds(u * half, half)
                for k, e in enumerate(es):
                    if final and e == 0:
                        last[at, :rows] = prod
                    else:
                        v2[e, g, at] = prod[k * half : (k + 1) * half, :]
                if 1 in es:
                    c_copy(v2.at[1, g, at], r3.at[g, at], g).start()

    def stage3(g):
        c_copy(v2.at[1, g], r3.at[g], g).wait_recv()
        third(jnp.concatenate([v2[0, g], r3[g]], axis=1), w3, dbuf, out, g * SG, (kb, jb, ni))

    def step(g, carry):
        for p in range(PIECES):
            stage1(g, p)
            if p == PIECES - 2:
                pl.when(g >= 2)(lambda: stage3(g - 2))
        pl.when(g + AHEAD < groups)(lambda: send_group(g + AHEAD))
        pl.when(g == 0)(build_rest)
        pl.when(g >= 1)(lambda: stage2(g - 1))
        return carry

    lax.fori_loop(0, groups, step, 0)
    stage3(groups - 2)
    stage2(groups - 1, True)
    c_copy(v2.at[1, groups - 1], r3.at[groups - 1], groups - 1).wait_recv()
    last[:, rows:] = r3[groups - 1]

    y_copy(tbuf.at[pl.ds(1, n3 - 1)], r1, 0).wait_send()
    x_copy(u3.at[pl.ds(1, n2 - 1)], r2, 0).wait_send()
    c_copy(v2.at[1], r3, 0).wait_send()


def solution(mesh):
    n3, n2, n1 = mesh.shape["m3"], mesh.shape["m2"], mesh.shape["m1"]

    def local_step(vol_blk, fac_one, fac_two, fac_three, diag_blk):
        ns, na, nb, nl = vol_blk.shape
        nk, nj, ni = fac_three.shape[0], fac_two.shape[0], fac_one.shape[0]
        kb, jb = nk // n2, nj // n1
        groups, rows = ns // n3 // SG, na * SG
        bl, bk, kj = nb * nl, nb * kb, kb * jb
        dims = (n3, n2, n1, na, nb, nl, ns, nk, nj, ni)
        dma = pltpu.SemaphoreType.DMA
        any_space = pl.BlockSpec(memory_space=pl.ANY)
        scratch = [
            pltpu.VMEM((na, nb, nl, ns), BF16),
            pltpu.VMEM((n3, groups, na // 2, 2 * SG, bl), BF16),
            pltpu.VMEM((n3 - 1, groups, na // 2, 2 * SG, bl), BF16),
            pltpu.VMEM((n2, groups, rows, bk), BF16),
            pltpu.VMEM((n2 - 1, groups, rows, bk), BF16),
            pltpu.VMEM((n1, groups, kj, rows), BF16),
            pltpu.VMEM((groups, kj, rows), BF16),
            pltpu.VMEM((n3 * LANES, n2 * LANES), BF16),
            pltpu.VMEM((n1 * kj * LANES // bk, n2 * LANES), BF16),
            pltpu.VMEM((ns, ns), BF16),
            pltpu.VMEM(fac_one.shape, BF16),
            pltpu.VMEM(fac_two.shape, BF16),
            pltpu.VMEM(fac_three.shape, BF16),
            dma((len(FIRST),)), dma((4,)), dma, dma((groups * PIECES,)), dma, dma((groups,)), dma, dma((groups,)),
        ]
        vmem = pl.BlockSpec(memory_space=pltpu.VMEM)
        held = pl.pallas_call(
            functools.partial(kernel, dims),
            out_shape=(
                pltpu.VMEM((ns // n3 - SG, kb, jb, ni), BF16),
                pltpu.VMEM((kj, n1 * rows), BF16),
                pltpu.VMEM((n1 * rows, SG * 2 * ni), BF16),
                pltpu.VMEM(diag_blk.shape, F32),
            ),
            in_specs=[any_space] * 5,
            out_specs=(vmem,) * 4,
            scratch_shapes=scratch,
            compiler_params=pltpu.CompilerParams(collective_id=0, has_side_effects=True, vmem_limit_bytes=50 * 1024 * 1024),
        )(jnp.transpose(vol_blk, (1, 2, 3, 0)), fac_one, fac_two, fac_three, diag_blk)
        return pl.pallas_call(
            finish,
            out_shape=jax.ShapeDtypeStruct((ns // n3, kb, jb, ni), BF16),
            in_specs=[vmem] * 4,
            out_specs=any_space,
            scratch_shapes=[pltpu.VMEM((SG, kb, jb, ni), BF16), dma((COPIES + 1,))],
            compiler_params=pltpu.CompilerParams(vmem_limit_bytes=12 * 1024 * 1024),
        )(*held)

    return jax.shard_map(local_step, mesh=mesh, in_specs=(P("dp", "m1", "m2", "m3"), P(), P(), P(), P("m2", "m1", None)), out_specs=P(("dp", "m3"), "m2", "m1", None), check_vma=False)
```

```python
import functools

import jax
import jax.numpy as jnp
from jax import lax
from jax.experimental import pallas as pl
from jax.experimental.pallas import tpu as pltpu
from jax.sharding import PartitionSpec as P

MESH = pl.DeviceIdType.MESH
BF16, F32 = jnp.bfloat16, jnp.float32
SG = 8
PIECES = 8
FIRST = (1, 1) + (2,) * 7
COPIES = 7
FIRST_SEND_AT = 0
SEND_AT, THIRD_AT = (2,), (3,)
AHEAD = 2
LANES = 128


def far_first(n):
    return sorted(range(1, n), key=lambda d: -min(d, n - d))


def dot(lhs, rhs, contract=((1,), (0,))):
    return lax.dot_general(lhs, rhs, (contract, ((), ())), preferred_element_type=F32)


def iota(shape, dim):
    return lax.broadcasted_iota(jnp.int32, shape, dim)


def onehot(cond):
    return jnp.where(cond, 1.0, 0.0).astype(BF16)


def third(lhs, w3, d_ref, out, base, shape, pairs=range(SG // 2)):
    ni = shape[-1]
    wide = w3.shape[1] // SG
    scale = d_ref[...].reshape(-1, ni)
    for q in pairs:
        prod = dot(lhs, w3[:, q * 2 * wide : (q + 1) * 2 * wide]).astype(BF16)
        for i in range(2):
            one = prod[:, i * wide : i * wide + ni].astype(F32)
            out[base + 2 * q + i] = (scale * one).astype(BF16).reshape(shape)


def finish(done, last, w3, d_ref, out, tail, sem):
    size = done.shape[0]
    chunk = size // COPIES
    copies = [pltpu.make_async_copy(done.at[pl.ds(i * chunk, chunk)], out.at[pl.ds(i * chunk, chunk)], sem.at[i]) for i in range(COPIES)]
    for c in copies:
        c.start()
    third(last[...], w3, d_ref, tail, 0, tail.shape[1:])
    copies.append(pltpu.make_async_copy(tail, out.at[pl.ds(size, SG)], sem.at[COPIES]))
    copies[-1].start()
    for c in copies:
        c.wait()


def kernel(dims, x_hbm, a1_hbm, a2_hbm, a3_hbm, d_hbm, out, last, w3, dbuf, xbuf, tbuf, r1, u3, r2, v2, r3, w1, w2, ident, a1, a2, a3,
           in_sem, fac_sem, y_send, y_recv, x_send, x_recv, c_send, c_recv):
    n3, n2, n1, na, nb, nl, ns, nk, nj, ni = dims
    me3, me2, me1 = lax.axis_index("m3"), lax.axis_index("m2"), lax.axis_index("m1")
    groups = ns // n3 // SG
    rows = na * SG
    pairs = na // 2
    ppp = pairs // PIECES
    prow = rows // PIECES
    kb, jb = nk // n2, nj // n1
    bl, bk, kj = nb * nl, nb * kb, kb * jb
    bt, kt = bl // LANES, bk // LANES
    bs, ks = nb // bt, kb // kt
    half = ks * jb

    loads, cuts = [], [0]
    for n in FIRST:
        part = pl.ds(2 * cuts[-1], 2 * n)
        loads.append(pltpu.make_async_copy(x_hbm.at[part], xbuf.at[part], in_sem.at[len(loads)]))
        cuts.append(cuts[-1] + n)
    facs = [pltpu.make_async_copy(s, t, fac_sem.at[i]) for i, (s, t) in enumerate(((a3_hbm, a3), (a2_hbm, a2), (a1_hbm, a1), (d_hbm, dbuf)))]
    loads[0].start()

    barrier = pltpu.get_barrier_semaphore()
    peers = 0
    for axis, me, n in (("m3", me3, n3), ("m2", me2, n2), ("m1", me1, n1)):
        for d in range(1, n):
            pl.semaphore_signal(barrier, inc=1, device_id={axis: lax.rem(me + d, n)}, device_id_type=MESH)
            peers += 1
    for f in loads[1:] + facs:
        f.start()

    def y_copy(src, dst, sem, d=1):
        return pltpu.make_async_remote_copy(src_ref=src, dst_ref=dst, send_sem=y_send, recv_sem=y_recv.at[sem],
                                            device_id={"m3": lax.rem(me3 + d, n3)}, device_id_type=MESH)

    def x_copy(src, dst, sem, d=1):
        return pltpu.make_async_remote_copy(src_ref=src, dst_ref=dst, send_sem=x_send, recv_sem=x_recv.at[sem],
                                            device_id={"m2": lax.rem(me2 + d, n2)}, device_id_type=MESH)

    def c_copy(src, dst, sem):
        return pltpu.make_async_remote_copy(src_ref=src, dst_ref=dst, send_sem=c_send, recv_sem=c_recv.at[sem],
                                            device_id={"m1": lax.rem(me1 + 1, n1)}, device_id_type=MESH)

    def send_pairs(g, lo, n):
        at = pl.ds(lo, n)
        for d in far_first(n3):
            y_copy(tbuf.at[d, g, at], r1.at[d - 1, g, at], g * PIECES + lo // ppp, d).start()

    def send_group(g, part=0, parts=1):
        for p in range(part * PIECES // parts, (part + 1) * PIECES // parts):
            send_pairs(g, p * ppp, ppp)

    sd = ns // n3
    r, c = iota((ns, ns), 0), iota((ns, ns), 1)
    ident[...] = onehot(c == lax.rem(r // sd + me3, n3) * sd + lax.rem(r, sd))

    def build_rest():
        for f in facs[1:]:
            f.wait()
        c = iota((n2 * nb, n2 * LANES), 1)
        pick = onehot(iota((n2 * nb, n2 * LANES), 0) == lax.rem(me2 - c // LANES + n2, n2) * nb + lax.rem(c, LANES) // ks)
        cols2 = dot(a2[...], pick).astype(BF16)
        r, c = iota((half, n2 * LANES), 0), iota((half, n2 * LANES), 1)
        same_k = r // jb == lax.rem(c, ks)
        for e in range(n1):
            r = iota((half, nj), 0)
            sel = onehot(iota((half, nj), 1) == lax.rem(me1 + e, n1) * jb + lax.rem(r, jb))
            w2[e * half : (e + 1) * half, :] = jnp.where(same_k, dot(sel, cols2), 0.0).astype(BF16)

        c = iota((ni, SG * wide), 1)
        pick = onehot(iota((ni, SG * wide), 0) == lax.rem(c, wide))
        cols1 = dot(a1[...], pick, ((0,), (0,))).astype(BF16)
        r, c = iota((rows, SG * wide), 0), iota((rows, SG * wide), 1)
        same_s = lax.rem(r, SG) == c // wide
        for e in range(n1):
            r = iota((rows, n1 * na), 0)
            sel = onehot(iota((rows, n1 * na), 1) == lax.rem(me1 + e, n1) * na + r // SG)
            w3[e * rows : (e + 1) * rows, :] = jnp.where(same_s, dot(sel, cols1), 0.0).astype(BF16)

    wide = 2 * ni
    eye = ident[...]
    for h, n in enumerate(FIRST):
        loads[h].wait()
        for ap in range(cuts[h], cuts[h + 1]):
            two = [dot(eye, xbuf[2 * ap + i].reshape(bl, ns), ((1,), (1,))).reshape(ns // SG, SG, bl) for i in range(2)]
            tbuf[:, :, ap] = jnp.stack(two, axis=1).reshape(n3, groups, 2 * SG, bl).astype(BF16)
        if h == 0:
            pl.semaphore_wait(barrier, peers)
        send_pairs(0, cuts[h], n)

    c = iota((nk, n2 * LANES), 1)
    k_of = lax.rem(c, LANES) // (LANES // kt) * ks + lax.rem(c, ks)
    pick = onehot(iota((nk, n2 * LANES), 0) == lax.rem(c // LANES + me2, n2) * kb + k_of)
    r, c = iota((LANES, n2 * LANES), 0), iota((LANES, n2 * LANES), 1)
    same_b = r // nl == lax.rem(c // ks, bs)
    facs[0].wait()
    cols3 = dot(a3[...], pick, ((0,), (0,))).astype(BF16)
    for d in range(n3):
        r = iota((LANES, n3 * nl), 0)
        sel = onehot(iota((LANES, n3 * nl), 1) == lax.rem(me3 - d + n3, n3) * nl + lax.rem(r, nl))
        w1[d * LANES : (d + 1) * LANES, :] = jnp.where(same_b, dot(sel, cols3), 0.0).astype(BF16)

    def stage1(g, p):
        at = pl.ds(p * ppp, ppp)
        y_copy(tbuf.at[pl.ds(1, n3 - 1), g, at], r1.at[:, g, at], g * PIECES + p).wait_recv()
        got = [tbuf[0, g, at].reshape(prow, bl)] + [r1[d, g, at].reshape(prow, bl) for d in range(n3 - 1)]
        lhs = [jnp.concatenate([v[:, t * LANES : (t + 1) * LANES] for v in got], axis=1) for t in range(bt)]
        prod = dot(jnp.concatenate(lhs, axis=0), w1[...])
        width = LANES // bt
        slot = iota((prow, LANES), 1) // width
        at = pl.ds(p * prow, prow)
        for d in range(n2):
            by_b = [prod[t * prow : (t + 1) * prow, d * LANES : (d + 1) * LANES] for t in range(bt)]
            for u in range(kt):
                tile = by_b[u]
                for t in range(bt):
                    if t != u:
                        tile = jnp.where(slot == t, pltpu.roll(by_b[t], (t - u) * width % LANES, 1), tile)
                u3[d, g, at, u * LANES : (u + 1) * LANES] = tile.astype(BF16)
        for d in far_first(n2):
            x_copy(u3.at[d, g, at], r2.at[d - 1, g, at], g, d).start()

    def second(g, u, es):
        got = [u3.at[0, g]] + [r2.at[d, g] for d in range(n2 - 1)]
        rhs = jnp.concatenate([v[:, u * LANES : (u + 1) * LANES] for v in got], axis=1)
        prod = dot(w2[es[0] * half : (es[-1] + 1) * half, :], rhs, ((1,), (1,))).astype(BF16)
        at = pl.ds(u * half, half)
        for k, e in enumerate(es):
            v2[e, g, at] = prod[k * half : (k + 1) * half, :]
        if 1 in es:
            c_copy(v2.at[1, g, at], r3.at[g, at], g).start()

    def stage2(g, u):
        if u == 0:
            x_copy(u3.at[pl.ds(1, n2 - 1), g], r2.at[:, g], g).wait_recv()
        second(g, u, tuple(range(n1)))

    def stage3(g, part=0, parts=1):
        if part == 0:
            c_copy(v2.at[1, g], r3.at[g], g).wait_recv()
        third(jnp.concatenate([v2[0, g], r3[g]], axis=1), w3, dbuf, out, g * SG, (kb, jb, ni), range(part * SG // 2 // parts, (part + 1) * SG // 2 // parts))

    def step(g, carry):
        def later(p, lag, act):
            pl.when(g >= lag)(lambda: act(g - lag))

        for p in range(PIECES):
            stage1(g, p)
            if p == 0:
                later(p, 2, lambda k: stage2(k, 1))
            if p == FIRST_SEND_AT:
                for k in range(1, AHEAD):
                    pl.when(g == 0)(functools.partial(send_group, k))
            if p in SEND_AT:
                pl.when(g + AHEAD < groups)(lambda: send_group(g + AHEAD, SEND_AT.index(p), len(SEND_AT)))
            if p in THIRD_AT:
                later(p, 3, lambda k: stage3(k, THIRD_AT.index(p), len(THIRD_AT)))
        pl.when(g == 0)(build_rest)
        later(p, 1, lambda k: stage2(k, 0))
        return carry

    lax.fori_loop(0, groups, step, 0)
    fin = groups - 1
    stage2(fin - 1, 1)
    stage3(fin - 2)
    stage3(fin - 1)
    x_copy(u3.at[pl.ds(1, n2 - 1), fin], r2.at[:, fin], fin).wait_recv()
    for es in ((1,), (0,)):
        for u in range(kt):
            second(fin, u, es)
    last[:, :rows] = v2[0, fin]
    c_copy(v2.at[1, fin], r3.at[fin], fin).wait_recv()
    last[:, rows:] = r3[fin]

    y_copy(tbuf.at[pl.ds(1, n3 - 1)], r1, 0).wait_send()
    x_copy(u3.at[pl.ds(1, n2 - 1)], r2, 0).wait_send()
    c_copy(v2.at[1], r3, 0).wait_send()


def scoped(dims, *refs):
    dma = pltpu.SemaphoreType.DMA
    n3, ns = dims[0], dims[6]
    groups = ns // n3 // SG
    pl.run_scoped(functools.partial(kernel, dims, *refs), dma((len(FIRST),)), dma((4,)), dma, dma((groups * PIECES,)), dma, dma((groups,)), dma, dma((groups,)))


def solution(mesh):
    n3, n2, n1 = mesh.shape["m3"], mesh.shape["m2"], mesh.shape["m1"]

    def local_step(vol_blk, fac_one, fac_two, fac_three, diag_blk):
        ns, na, nb, nl = vol_blk.shape
        nk, nj, ni = fac_three.shape[0], fac_two.shape[0], fac_one.shape[0]
        kb, jb = nk // n2, nj // n1
        groups, rows = ns // n3 // SG, na * SG
        bl, bk, kj = nb * nl, nb * kb, kb * jb
        dims = (n3, n2, n1, na, nb, nl, ns, nk, nj, ni)
        dma = pltpu.SemaphoreType.DMA
        any_space = pl.BlockSpec(memory_space=pl.ANY)
        scratch = [
            pltpu.VMEM((na, nb, nl, ns), BF16),
            pltpu.VMEM((n3, groups, na // 2, 2 * SG, bl), BF16),
            pltpu.VMEM((n3 - 1, groups, na // 2, 2 * SG, bl), BF16),
            pltpu.VMEM((n2, groups, rows, bk), BF16),
            pltpu.VMEM((n2 - 1, groups, rows, bk), BF16),
            pltpu.VMEM((n1, groups, kj, rows), BF16),
            pltpu.VMEM((groups, kj, rows), BF16),
            pltpu.VMEM((n3 * LANES, n2 * LANES), BF16),
            pltpu.VMEM((n1 * kj * LANES // bk, n2 * LANES), BF16),
            pltpu.VMEM((ns, ns), BF16),
            pltpu.VMEM(fac_one.shape, BF16),
            pltpu.VMEM(fac_two.shape, BF16),
            pltpu.VMEM(fac_three.shape, BF16),
        ]
        vmem = pl.BlockSpec(memory_space=pltpu.VMEM)
        held = pl.pallas_call(
            functools.partial(scoped, dims),
            out_shape=(
                pltpu.VMEM((ns // n3 - SG, kb, jb, ni), BF16),
                pltpu.VMEM((kj, n1 * rows), BF16),
                pltpu.VMEM((n1 * rows, SG * 2 * ni), BF16),
                pltpu.VMEM(diag_blk.shape, F32),
            ),
            in_specs=[any_space] * 5,
            out_specs=(vmem,) * 4,
            scratch_shapes=scratch,
            compiler_params=pltpu.CompilerParams(collective_id=0, has_side_effects=True, vmem_limit_bytes=50 * 1024 * 1024),
        )(jnp.transpose(vol_blk, (1, 2, 3, 0)), fac_one, fac_two, fac_three, diag_blk)
        return pl.pallas_call(
            finish,
            out_shape=jax.ShapeDtypeStruct((ns // n3, kb, jb, ni), BF16),
            in_specs=[vmem] * 4,
            out_specs=any_space,
            scratch_shapes=[pltpu.VMEM((SG, kb, jb, ni), BF16), dma((COPIES + 1,))],
            compiler_params=pltpu.CompilerParams(vmem_limit_bytes=12 * 1024 * 1024),
        )(*held)

    return jax.shard_map(local_step, mesh=mesh, in_specs=(P("dp", "m1", "m2", "m3"), P(), P(), P(), P("m2", "m1", None)), out_specs=P(("dp", "m3"), "m2", "m1", None), check_vma=False)
```

```python
import functools

import jax
import jax.numpy as jnp
from jax import lax
from jax.experimental import pallas as pl
from jax.experimental.pallas import tpu as pltpu
from jax.sharding import PartitionSpec as P

MESH = pl.DeviceIdType.MESH
BF16, F32 = jnp.bfloat16, jnp.float32
SG = 8
SIZES = (2,) * 8
PIECES = len(SIZES)
STARTS = tuple(sum(SIZES[:i]) for i in range(PIECES))
FIRST = (1, 1, 2, 4, 4, 4)
COPIES = 6
LATE = 2
FIRST_SEND_AT = 2
SEND_AT, THIRD_AT = (5,), (3,)
AHEAD = 2
LANES = 128


def far_first(n):
    return sorted(range(1, n), key=lambda d: -min(d, n - d))


def dot(lhs, rhs, contract=((1,), (0,))):
    return lax.dot_general(lhs, rhs, (contract, ((), ())), preferred_element_type=F32)


def iota(shape, dim):
    return lax.broadcasted_iota(jnp.int32, shape, dim)


def onehot(cond):
    return jnp.where(cond, 1.0, 0.0).astype(BF16)


def third(lhs, w3, d_ref, out, base, shape, pairs=range(SG // 2)):
    ni = shape[-1]
    wide = w3.shape[1] // SG
    scale = d_ref[...].reshape(-1, ni)
    for q in pairs:
        prod = dot(lhs, w3[:, q * 2 * wide : (q + 1) * 2 * wide]).astype(BF16)
        for i in range(2):
            one = prod[:, i * wide : i * wide + ni].astype(F32)
            out[base + 2 * q + i] = (scale * one).astype(BF16).reshape(shape)


def finish(done, last, w3, d_ref, out, tail, sem):
    size = done.shape[0]
    chunk = size // COPIES
    copies = [pltpu.make_async_copy(done.at[pl.ds(i * chunk, chunk)], out.at[pl.ds(i * chunk, chunk)], sem.at[i]) for i in range(COPIES)]
    for c in copies:
        c.start()
    for k in range(LATE):
        third(last[k], w3, d_ref, tail, k * SG, tail.shape[1:])
        copies.append(pltpu.make_async_copy(tail.at[pl.ds(k * SG, SG)], out.at[pl.ds(size + k * SG, SG)], sem.at[COPIES + k]))
        copies[-1].start()
    for c in copies:
        c.wait()


def kernel(dims, x_hbm, a1_hbm, a2_hbm, a3_hbm, d_hbm, out, last, w3, dbuf, xbuf, tbuf, r1, u3, r2, v2, r3, w1, w2, ident, a1, a2, a3,
           in_sem, fac_sem, y_send, y_recv, x_send, x_recv, c_send, c_recv):
    n3, n2, n1, na, nb, nl, ns, nk, nj, ni = dims
    me3, me2, me1 = lax.axis_index("m3"), lax.axis_index("m2"), lax.axis_index("m1")
    groups = ns // n3 // SG
    rows = na * SG
    pairs = na // 2
    kb, jb = nk // n2, nj // n1
    bl, bk, kj = nb * nl, nb * kb, kb * jb
    bt, kt = bl // LANES, bk // LANES
    bs, ks = nb // bt, kb // kt
    half = ks * jb

    loads, cuts = [], [0]
    for n in FIRST:
        part = pl.ds(2 * cuts[-1], 2 * n)
        loads.append(pltpu.make_async_copy(x_hbm.at[part], xbuf.at[part], in_sem.at[len(loads)]))
        cuts.append(cuts[-1] + n)
    facs = [pltpu.make_async_copy(s, t, fac_sem.at[i]) for i, (s, t) in enumerate(((a3_hbm, a3), (a2_hbm, a2), (a1_hbm, a1), (d_hbm, dbuf)))]
    loads[0].start()

    barrier = pltpu.get_barrier_semaphore()
    peers = 0
    other = lax.rem(me1 + 1, n1)
    for axis, me, n, core, first in (("m3", me3, n3, me1, 1), ("m2", me2, n2, other, 0)):
        for d in range(first, n):
            pl.semaphore_signal(barrier, inc=1, device_id={axis: lax.rem(me + d, n), "m1": core}, device_id_type=MESH)
            peers += 1
    for f in loads[1:] + facs:
        f.start()

    def y_copy(src, dst, sem, d=1):
        return pltpu.make_async_remote_copy(src_ref=src, dst_ref=dst, send_sem=y_send, recv_sem=y_recv.at[sem],
                                            device_id={"m3": lax.rem(me3 + d, n3)}, device_id_type=MESH)

    def x_copy(src, dst, sem, d=1):
        return pltpu.make_async_remote_copy(src_ref=src, dst_ref=dst, send_sem=x_send, recv_sem=x_recv.at[sem],
                                            device_id={"m2": lax.rem(me2 + d, n2), "m1": other}, device_id_type=MESH)

    def c_copy(src, dst, sem):
        return pltpu.make_async_remote_copy(src_ref=src, dst_ref=dst, send_sem=c_send, recv_sem=c_recv.at[sem],
                                            device_id={"m1": other}, device_id_type=MESH)

    def send_pairs(g, lo, n, p):
        at = pl.ds(lo, n)
        for d in far_first(n3):
            y_copy(tbuf.at[d, g, at], r1.at[d - 1, g, at], g * PIECES + p, d).start()

    def send_group(g, part=0, parts=1):
        for p in range(part * PIECES // parts, (part + 1) * PIECES // parts):
            send_pairs(g, STARTS[p], SIZES[p], p)

    sd = ns // n3
    r, c = iota((ns, ns), 0), iota((ns, ns), 1)
    ident[...] = onehot(c == lax.rem(r // sd + me3, n3) * sd + lax.rem(r, sd))

    def build_rest():
        for f in facs[1:]:
            f.wait()
        c = iota((n2 * nb, n2 * LANES), 1)
        pick = onehot(iota((n2 * nb, n2 * LANES), 0) == lax.rem(me2 - c // LANES + n2, n2) * nb + lax.rem(c, LANES) // ks)
        cols2 = dot(a2[...], pick).astype(BF16)
        r, c = iota((half, n2 * LANES), 0), iota((half, n2 * LANES), 1)
        same_k = r // jb == lax.rem(c, ks)
        for e in range(n1):
            r = iota((half, nj), 0)
            sel = onehot(iota((half, nj), 1) == lax.rem(me1 + e, n1) * jb + lax.rem(r, jb))
            w2[e * half : (e + 1) * half, :] = jnp.where(same_k, dot(sel, cols2), 0.0).astype(BF16)

        c = iota((ni, SG * wide), 1)
        pick = onehot(iota((ni, SG * wide), 0) == lax.rem(c, wide))
        cols1 = dot(a1[...], pick, ((0,), (0,))).astype(BF16)
        r, c = iota((rows, SG * wide), 0), iota((rows, SG * wide), 1)
        same_s = lax.rem(r, SG) == c // wide
        for e in range(n1):
            r = iota((rows, n1 * na), 0)
            sel = onehot(iota((rows, n1 * na), 1) == lax.rem(me1 + 1 + e, n1) * na + r // SG)
            w3[e * rows : (e + 1) * rows, :] = jnp.where(same_s, dot(sel, cols1), 0.0).astype(BF16)

    wide = 2 * ni
    eye = ident[...]
    for h, n in enumerate(FIRST):
        loads[h].wait()
        for ap in range(cuts[h], cuts[h + 1]):
            two = [dot(eye, xbuf[2 * ap + i].reshape(bl, ns), ((1,), (1,))).reshape(ns // SG, SG, bl) for i in range(2)]
            tbuf[:, :, ap] = jnp.stack(two, axis=1).reshape(n3, groups, 2 * SG, bl).astype(BF16)
        if h == 0:
            pl.semaphore_wait(barrier, peers)
        for p in range(PIECES):
            lo, hi = max(cuts[h], STARTS[p]), min(cuts[h + 1], STARTS[p] + SIZES[p])
            if lo < hi:
                send_pairs(0, lo, hi - lo, p)

    c = iota((nk, n2 * LANES), 1)
    k_of = lax.rem(c, LANES) // (LANES // kt) * ks + lax.rem(c, ks)
    pick = onehot(iota((nk, n2 * LANES), 0) == lax.rem(c // LANES + me2, n2) * kb + k_of)
    r, c = iota((LANES, n2 * LANES), 0), iota((LANES, n2 * LANES), 1)
    same_b = r // nl == lax.rem(c // ks, bs)
    facs[0].wait()
    cols3 = dot(a3[...], pick, ((0,), (0,))).astype(BF16)
    for d in range(n3):
        r = iota((LANES, n3 * nl), 0)
        sel = onehot(iota((LANES, n3 * nl), 1) == lax.rem(me3 - d + n3, n3) * nl + lax.rem(r, nl))
        w1[d * LANES : (d + 1) * LANES, :] = jnp.where(same_b, dot(sel, cols3), 0.0).astype(BF16)

    def stage1(g, p):
        at, prow = pl.ds(STARTS[p], SIZES[p]), 2 * SG * SIZES[p]
        y_copy(tbuf.at[pl.ds(1, n3 - 1), g, at], r1.at[:, g, at], g * PIECES + p).wait_recv()
        got = [tbuf[0, g, at].reshape(prow, bl)] + [r1[d, g, at].reshape(prow, bl) for d in range(n3 - 1)]
        lhs = [jnp.concatenate([v[:, t * LANES : (t + 1) * LANES] for v in got], axis=1) for t in range(bt)]
        prod = dot(jnp.concatenate(lhs, axis=0), w1[...])
        width = LANES // bt
        slot = iota((prow, LANES), 1) // width
        at = pl.ds(STARTS[p] * 2 * SG, prow)
        for d in range(n2):
            by_b = [prod[t * prow : (t + 1) * prow, d * LANES : (d + 1) * LANES] for t in range(bt)]
            for u in range(kt):
                tile = by_b[u]
                for t in range(bt):
                    if t != u:
                        tile = jnp.where(slot == t, pltpu.roll(by_b[t], (t - u) * width % LANES, 1), tile)
                u3[d, g, at, u * LANES : (u + 1) * LANES] = tile.astype(BF16)
        for d in (*far_first(n2), 0):
            x_copy(u3.at[d, g, at], r2.at[d, g, at], 2 * g + 2 * p // PIECES, d).start()

    def x_wait(g, part):
        at = pl.ds(part * rows // 2, rows // 2)
        x_copy(u3.at[:, g, at], r2.at[:, g, at], 2 * g + part).wait_recv()

    def second(g, u, es, col=slice(None), send=True):
        got = [r2.at[d, g, col] for d in range(n2)]
        rhs = jnp.concatenate([v[:, u * LANES : (u + 1) * LANES] for v in got], axis=1)
        prod = dot(w2[es[0] * half : (es[-1] + 1) * half, :], rhs, ((1,), (1,))).astype(BF16)
        at = pl.ds(u * half, half)
        for k, e in enumerate(es):
            v2[e, g, at, col] = prod[k * half : (k + 1) * half, :]
        if 1 in es and send:
            c_copy(v2.at[1, g, at, col], r3.at[g, at, col], g).start()

    def stage2(g, u):
        if u == 0:
            for part in range(2):
                x_wait(g, part)
        second(g, u, tuple(range(n1)))

    def stage3(g, part=0, parts=1):
        if part == 0:
            c_copy(v2.at[1, g], r3.at[g], g).wait_recv()
        third(jnp.concatenate([v2[0, g], r3[g]], axis=1), w3, dbuf, out, g * SG, (kb, jb, ni), range(part * SG // 2 // parts, (part + 1) * SG // 2 // parts))

    def step(g, carry):
        def later(p, lag, act):
            pl.when(g >= lag)(lambda: act(g - lag))

        for p in range(PIECES):
            stage1(g, p)
            if p == 0:
                later(p, 2, lambda k: stage2(k, 1))
            if p == FIRST_SEND_AT:
                for k in range(1, AHEAD):
                    pl.when(g == 0)(functools.partial(send_group, k))
            if p in SEND_AT:
                pl.when(g + AHEAD < groups)(lambda: send_group(g + AHEAD, SEND_AT.index(p), len(SEND_AT)))
            if p in THIRD_AT:
                later(p, 3, lambda k: stage3(k, THIRD_AT.index(p), len(THIRD_AT)))
        pl.when(g == 0)(build_rest)
        later(p, 1, lambda k: stage2(k, 0))
        return carry

    lax.fori_loop(0, groups, step, 0)
    fin = groups - 1
    stage2(fin - 1, 1)
    stage3(fin - 2)
    def hand_over(g):
        c_copy(v2.at[1, g], r3.at[g], g).wait_recv()
        last[g - groups + LATE, :, :rows] = v2[0, g]
        last[g - groups + LATE, :, rows:] = r3[g]

    for part in range(2):
        x_wait(fin, part)
        col = pl.ds(part * rows // 2, rows // 2)
        for u in range(kt):
            second(fin, u, (1,), col, False)
        c_copy(v2.at[1, fin, :, col], r3.at[fin, :, col], fin).start()
        if part == 0:
            hand_over(fin - 1)
    for u in range(kt):
        second(fin, u, (0,))
    hand_over(fin)

    y_copy(tbuf.at[pl.ds(1, n3 - 1)], r1, 0).wait_send()
    x_copy(u3, r2, 0).wait_send()
    c_copy(v2.at[1], r3, 0).wait_send()


def scoped(dims, *refs):
    dma = pltpu.SemaphoreType.DMA
    n3, ns = dims[0], dims[6]
    groups = ns // n3 // SG
    pl.run_scoped(functools.partial(kernel, dims, *refs), dma((len(FIRST),)), dma((4,)), dma, dma((groups * PIECES,)), dma, dma((2 * groups,)), dma, dma((groups,)))


def solution(mesh):
    n3, n2, n1 = mesh.shape["m3"], mesh.shape["m2"], mesh.shape["m1"]

    def local_step(vol_blk, fac_one, fac_two, fac_three, diag_blk):
        ns, na, nb, nl = vol_blk.shape
        nk, nj, ni = fac_three.shape[0], fac_two.shape[0], fac_one.shape[0]
        kb, jb = nk // n2, nj // n1
        groups, rows = ns // n3 // SG, na * SG
        bl, bk, kj = nb * nl, nb * kb, kb * jb
        dims = (n3, n2, n1, na, nb, nl, ns, nk, nj, ni)
        dma = pltpu.SemaphoreType.DMA
        any_space = pl.BlockSpec(memory_space=pl.ANY)
        scratch = [
            pltpu.VMEM((na, nb, nl, ns), BF16),
            pltpu.VMEM((n3, groups, na // 2, 2 * SG, bl), BF16),
            pltpu.VMEM((n3 - 1, groups, na // 2, 2 * SG, bl), BF16),
            pltpu.VMEM((n2, groups, rows, bk), BF16),
            pltpu.VMEM((n2, groups, rows, bk), BF16),
            pltpu.VMEM((n1, groups, kj, rows), BF16),
            pltpu.VMEM((groups, kj, rows), BF16),
            pltpu.VMEM((n3 * LANES, n2 * LANES), BF16),
            pltpu.VMEM((n1 * kj * LANES // bk, n2 * LANES), BF16),
            pltpu.VMEM((ns, ns), BF16),
            pltpu.VMEM(fac_one.shape, BF16),
            pltpu.VMEM(fac_two.shape, BF16),
            pltpu.VMEM(fac_three.shape, BF16),
        ]
        vmem = pl.BlockSpec(memory_space=pltpu.VMEM)
        held = pl.pallas_call(
            functools.partial(scoped, dims),
            out_shape=(
                pltpu.VMEM((ns // n3 - LATE * SG, kb, jb, ni), BF16),
                pltpu.VMEM((LATE, kj, n1 * rows), BF16),
                pltpu.VMEM((n1 * rows, SG * 2 * ni), BF16),
                pltpu.VMEM(diag_blk.shape, F32),
            ),
            in_specs=[any_space] * 5,
            out_specs=(vmem,) * 4,
            scratch_shapes=scratch,
            compiler_params=pltpu.CompilerParams(collective_id=0, has_side_effects=True, vmem_limit_bytes=50 * 1024 * 1024),
        )(jnp.transpose(vol_blk, (1, 2, 3, 0)), fac_one, fac_two, fac_three, diag_blk)
        return pl.pallas_call(
            finish,
            out_shape=jax.ShapeDtypeStruct((ns // n3, kb, jb, ni), BF16),
            in_specs=[vmem] * 4,
            out_specs=any_space,
            scratch_shapes=[pltpu.VMEM((LATE * SG, kb, jb, ni), BF16), dma((COPIES + LATE,))],
            compiler_params=pltpu.CompilerParams(vmem_limit_bytes=12 * 1024 * 1024),
        )(*held)

    return jax.shard_map(local_step, mesh=mesh, in_specs=(P("dp", "m1", "m2", "m3"), P(), P(), P(), P("m2", "m1", None)), out_specs=P(("dp", "m3"), "m2", "m1", None), check_vma=False)
```

```python
import functools

import jax
import jax.numpy as jnp
from jax import lax
from jax.experimental import pallas as pl
from jax.experimental.pallas import tpu as pltpu
from jax.sharding import PartitionSpec as P

MESH = pl.DeviceIdType.MESH
BF16, F32 = jnp.bfloat16, jnp.float32
SG = 8
SIZES = (2,) * 8
PIECES = len(SIZES)
STARTS = tuple(sum(SIZES[:i]) for i in range(PIECES))
FIRST = (1, 1, 2, 4, 4, 4)
COPIES = 3
LATE = 2
FIRST_SEND_AT = 2
SEND_AT, THIRD_AT = (5, 6), (2, 3)
AHEAD = 2
LANES = 128


def far_first(n):
    return sorted(range(1, n), key=lambda d: -min(d, n - d))


def dot(lhs, rhs, contract=((1,), (0,))):
    return lax.dot_general(lhs, rhs, (contract, ((), ())), preferred_element_type=F32)


def iota(shape, dim):
    return lax.broadcasted_iota(jnp.int32, shape, dim)


def onehot(cond):
    return jnp.where(cond, 1.0, 0.0).astype(BF16)


def third(lhs, w3, d_ref, out, base, shape, pairs=range(SG // 2)):
    ni = shape[-1]
    wide = w3.shape[1] // SG
    scale = d_ref[...].reshape(-1, ni)
    for q in pairs:
        prod = dot(lhs, w3[:, q * 2 * wide : (q + 1) * 2 * wide]).astype(BF16)
        for i in range(2):
            one = prod[:, i * wide : i * wide + ni].astype(F32)
            out[base + 2 * q + i] = (scale * one).astype(BF16).reshape(shape)


def finish(done, last, w3, d_ref, out, tail, sem):
    size = done.shape[0]
    chunk = size // COPIES
    copies = [pltpu.make_async_copy(done.at[pl.ds(i * chunk, chunk)], out.at[pl.ds(i * chunk, chunk)], sem.at[i]) for i in range(COPIES)]
    for c in copies:
        c.start()
    for k in range(LATE):
        third(last[k], w3, d_ref, tail, k * SG, tail.shape[1:])
        copies.append(pltpu.make_async_copy(tail.at[pl.ds(k * SG, SG)], out.at[pl.ds(size + k * SG, SG)], sem.at[COPIES + k]))
        copies[-1].start()
    for c in copies:
        c.wait()


def kernel(dims, x_hbm, a1_hbm, a2_hbm, a3_hbm, d_hbm, out, last, w3, dbuf, xbuf, tbuf, r1, u3, r2, v2, r3, w1, w2, ident, a1, a2, a3,
           in_sem, fac_sem, y_send, y_recv, x_send, x_recv, c_send, c_recv):
    n3, n2, n1, na, nb, nl, ns, nk, nj, ni = dims
    me3, me2, me1 = lax.axis_index("m3"), lax.axis_index("m2"), lax.axis_index("m1")
    groups = ns // n3 // SG
    rows = na * SG
    pairs = na // 2
    kb, jb = nk // n2, nj // n1
    bl, bk, kj = nb * nl, nb * kb, kb * jb
    bt, kt = bl // LANES, bk // LANES
    bs, ks = nb // bt, kb // kt
    half = ks * jb

    loads, cuts = [], [0]
    for n in FIRST:
        part = pl.ds(2 * cuts[-1], 2 * n)
        loads.append(pltpu.make_async_copy(x_hbm.at[part], xbuf.at[part], in_sem.at[len(loads)]))
        cuts.append(cuts[-1] + n)
    facs = [pltpu.make_async_copy(s, t, fac_sem.at[i]) for i, (s, t) in enumerate(((a3_hbm, a3), (a2_hbm, a2), (a1_hbm, a1), (d_hbm, dbuf)))]
    loads[0].start()

    barrier = pltpu.get_barrier_semaphore()
    peers = 0
    other = lax.rem(me1 + 1, n1)
    for axis, me, n, core, first in (("m3", me3, n3, me1, 1), ("m2", me2, n2, other, 0)):
        for d in range(first, n):
            pl.semaphore_signal(barrier, inc=1, device_id={axis: lax.rem(me + d, n), "m1": core}, device_id_type=MESH)
            peers += 1
    for f in loads[1:] + facs:
        f.start()

    def y_copy(src, dst, sem, d=1):
        return pltpu.make_async_remote_copy(src_ref=src, dst_ref=dst, send_sem=y_send, recv_sem=y_recv.at[sem],
                                            device_id={"m3": lax.rem(me3 + d, n3)}, device_id_type=MESH)

    def x_copy(src, dst, sem, d=1):
        return pltpu.make_async_remote_copy(src_ref=src, dst_ref=dst, send_sem=x_send, recv_sem=x_recv.at[sem],
                                            device_id={"m2": lax.rem(me2 + d, n2), "m1": other}, device_id_type=MESH)

    def c_copy(src, dst, sem):
        return pltpu.make_async_remote_copy(src_ref=src, dst_ref=dst, send_sem=c_send, recv_sem=c_recv.at[sem],
                                            device_id={"m1": other}, device_id_type=MESH)

    def send_pairs(g, lo, n, p):
        at = pl.ds(lo, n)
        for d in far_first(n3):
            y_copy(tbuf.at[d, g, at], r1.at[d - 1, g, at], g * PIECES + p, d).start()

    def send_group(g, part=0, parts=1):
        for p in range(part * PIECES // parts, (part + 1) * PIECES // parts):
            send_pairs(g, STARTS[p], SIZES[p], p)

    sd = ns // n3
    r, c = iota((ns, ns), 0), iota((ns, ns), 1)
    ident[...] = onehot(c == lax.rem(r // sd + me3, n3) * sd + lax.rem(r, sd))

    def build_rest():
        for f in facs[1:]:
            f.wait()
        c = iota((n2 * nb, n2 * LANES), 1)
        pick = onehot(iota((n2 * nb, n2 * LANES), 0) == lax.rem(me2 - c // LANES + n2, n2) * nb + lax.rem(c, LANES) // ks)
        cols2 = dot(a2[...], pick).astype(BF16)
        r, c = iota((half, n2 * LANES), 0), iota((half, n2 * LANES), 1)
        same_k = r // jb == lax.rem(c, ks)
        for e in range(n1):
            r = iota((half, nj), 0)
            sel = onehot(iota((half, nj), 1) == lax.rem(me1 + e, n1) * jb + lax.rem(r, jb))
            w2[e * half : (e + 1) * half, :] = jnp.where(same_k, dot(sel, cols2), 0.0).astype(BF16)

        c = iota((ni, SG * wide), 1)
        pick = onehot(iota((ni, SG * wide), 0) == lax.rem(c, wide))
        cols1 = dot(a1[...], pick, ((0,), (0,))).astype(BF16)
        r, c = iota((rows, SG * wide), 0), iota((rows, SG * wide), 1)
        same_s = lax.rem(r, SG) == c // wide
        for e in range(n1):
            r = iota((rows, n1 * na), 0)
            sel = onehot(iota((rows, n1 * na), 1) == lax.rem(me1 + 1 + e, n1) * na + r // SG)
            w3[e * rows : (e + 1) * rows, :] = jnp.where(same_s, dot(sel, cols1), 0.0).astype(BF16)

    wide = 2 * ni
    eye = ident[...]
    for h, n in enumerate(FIRST):
        loads[h].wait()
        for ap in range(cuts[h], cuts[h + 1]):
            two = [dot(eye, xbuf[2 * ap + i].reshape(bl, ns), ((1,), (1,))).reshape(ns // SG, SG, bl) for i in range(2)]
            tbuf[:, :, ap] = jnp.stack(two, axis=1).reshape(n3, groups, 2 * SG, bl).astype(BF16)
        if h == 0:
            pl.semaphore_wait(barrier, peers)
        for p in range(PIECES):
            lo, hi = max(cuts[h], STARTS[p]), min(cuts[h + 1], STARTS[p] + SIZES[p])
            if lo < hi:
                send_pairs(0, lo, hi - lo, p)

    c = iota((nk, n2 * LANES), 1)
    k_of = lax.rem(c, LANES) // (LANES // kt) * ks + lax.rem(c, ks)
    pick = onehot(iota((nk, n2 * LANES), 0) == lax.rem(c // LANES + me2, n2) * kb + k_of)
    r, c = iota((LANES, n2 * LANES), 0), iota((LANES, n2 * LANES), 1)
    same_b = r // nl == lax.rem(c // ks, bs)
    facs[0].wait()
    cols3 = dot(a3[...], pick, ((0,), (0,))).astype(BF16)
    for d in range(n3):
        r = iota((LANES, n3 * nl), 0)
        sel = onehot(iota((LANES, n3 * nl), 1) == lax.rem(me3 - d + n3, n3) * nl + lax.rem(r, nl))
        w1[d * LANES : (d + 1) * LANES, :] = jnp.where(same_b, dot(sel, cols3), 0.0).astype(BF16)

    def stage1(g, p):
        at, prow = pl.ds(STARTS[p], SIZES[p]), 2 * SG * SIZES[p]
        y_copy(tbuf.at[pl.ds(1, n3 - 1), g, at], r1.at[:, g, at], g * PIECES + p).wait_recv()
        got = [tbuf[0, g, at].reshape(prow, bl)] + [r1[d, g, at].reshape(prow, bl) for d in range(n3 - 1)]
        lhs = [jnp.concatenate([v[:, t * LANES : (t + 1) * LANES] for v in got], axis=1) for t in range(bt)]
        prod = dot(jnp.concatenate(lhs, axis=0), w1[...])
        width = LANES // bt
        slot = iota((prow, LANES), 1) // width
        at = pl.ds(STARTS[p] * 2 * SG, prow)
        for d in range(n2):
            by_b = [prod[t * prow : (t + 1) * prow, d * LANES : (d + 1) * LANES] for t in range(bt)]
            for u in range(kt):
                tile = by_b[u]
                for t in range(bt):
                    if t != u:
                        tile = jnp.where(slot == t, pltpu.roll(by_b[t], (t - u) * width % LANES, 1), tile)
                u3[d, g, at, u * LANES : (u + 1) * LANES] = tile.astype(BF16)
        for d in (*far_first(n2), 0):
            x_copy(u3.at[d, g, at], r2.at[d, g, at], 2 * g + 2 * STARTS[p] // pairs, d).start()

    def x_wait(g, part):
        at = pl.ds(part * rows // 2, rows // 2)
        x_copy(u3.at[:, g, at], r2.at[:, g, at], 2 * g + part).wait_recv()

    def second(g, u, es, col=slice(None), send=True):
        got = [r2.at[d, g, col] for d in range(n2)]
        rhs = jnp.concatenate([v[:, u * LANES : (u + 1) * LANES] for v in got], axis=1)
        prod = dot(w2[es[0] * half : (es[-1] + 1) * half, :], rhs, ((1,), (1,))).astype(BF16)
        at = pl.ds(u * half, half)
        for k, e in enumerate(es):
            v2[e, g, at, col] = prod[k * half : (k + 1) * half, :]
        if 1 in es and send:
            c_copy(v2.at[1, g, at, col], r3.at[g, at, col], g).start()

    def stage2(g, u):
        if u == 0:
            for part in range(2):
                x_wait(g, part)
        second(g, u, tuple(range(n1)))

    def stage3(g, part=0, parts=1):
        if part == 0:
            c_copy(v2.at[1, g], r3.at[g], g).wait_recv()
        third(jnp.concatenate([v2[0, g], r3[g]], axis=1), w3, dbuf, out, g * SG, (kb, jb, ni), range(part * SG // 2 // parts, (part + 1) * SG // 2 // parts))

    def step(g, carry):
        def later(p, lag, act):
            pl.when(g >= lag)(lambda: act(g - lag))

        for p in range(PIECES):
            stage1(g, p)
            if p == 0:
                later(p, 2, lambda k: stage2(k, 1))
            if p == FIRST_SEND_AT:
                for k in range(1, AHEAD):
                    pl.when(g == 0)(functools.partial(send_group, k))
            if p in SEND_AT:
                pl.when(g + AHEAD < groups)(lambda: send_group(g + AHEAD, SEND_AT.index(p), len(SEND_AT)))
            if p in THIRD_AT:
                later(p, 3, lambda k: stage3(k, THIRD_AT.index(p), len(THIRD_AT)))
        pl.when(g == 0)(build_rest)
        later(p, 1, lambda k: stage2(k, 0))
        return carry

    lax.fori_loop(0, groups, step, 0)
    fin = groups - 1
    stage2(fin - 1, 1)
    stage3(fin - 2)
    def hand_over(g):
        c_copy(v2.at[1, g], r3.at[g], g).wait_recv()
        last[g - groups + LATE, :, :rows] = v2[0, g]
        last[g - groups + LATE, :, rows:] = r3[g]

    for part in range(2):
        x_wait(fin, part)
        col = pl.ds(part * rows // 2, rows // 2)
        for u in range(kt):
            second(fin, u, (1,), col, False)
        c_copy(v2.at[1, fin, :, col], r3.at[fin, :, col], fin).start()
        if part == 0:
            hand_over(fin - 1)
    for u in range(kt):
        second(fin, u, (0,))
    hand_over(fin)

    y_copy(tbuf.at[pl.ds(1, n3 - 1)], r1, 0).wait_send()
    x_copy(u3, r2, 0).wait_send()
    c_copy(v2.at[1], r3, 0).wait_send()


def scoped(dims, *refs):
    dma = pltpu.SemaphoreType.DMA
    n3, ns = dims[0], dims[6]
    groups = ns // n3 // SG
    pl.run_scoped(functools.partial(kernel, dims, *refs), dma((len(FIRST),)), dma((4,)), dma, dma((groups * PIECES,)), dma, dma((2 * groups,)), dma, dma((groups,)))


def solution(mesh):
    n3, n2, n1 = mesh.shape["m3"], mesh.shape["m2"], mesh.shape["m1"]

    def local_step(vol_blk, fac_one, fac_two, fac_three, diag_blk):
        ns, na, nb, nl = vol_blk.shape
        nk, nj, ni = fac_three.shape[0], fac_two.shape[0], fac_one.shape[0]
        kb, jb = nk // n2, nj // n1
        groups, rows = ns // n3 // SG, na * SG
        bl, bk, kj = nb * nl, nb * kb, kb * jb
        dims = (n3, n2, n1, na, nb, nl, ns, nk, nj, ni)
        dma = pltpu.SemaphoreType.DMA
        any_space = pl.BlockSpec(memory_space=pl.ANY)
        scratch = [
            pltpu.VMEM((na, nb, nl, ns), BF16),
            pltpu.VMEM((n3, groups, na // 2, 2 * SG, bl), BF16),
            pltpu.VMEM((n3 - 1, groups, na // 2, 2 * SG, bl), BF16),
            pltpu.VMEM((n2, groups, rows, bk), BF16),
            pltpu.VMEM((n2, groups, rows, bk), BF16),
            pltpu.VMEM((n1, groups, kj, rows), BF16),
            pltpu.VMEM((groups, kj, rows), BF16),
            pltpu.VMEM((n3 * LANES, n2 * LANES), BF16),
            pltpu.VMEM((n1 * kj * LANES // bk, n2 * LANES), BF16),
            pltpu.VMEM((ns, ns), BF16),
            pltpu.VMEM(fac_one.shape, BF16),
            pltpu.VMEM(fac_two.shape, BF16),
            pltpu.VMEM(fac_three.shape, BF16),
        ]
        vmem = pl.BlockSpec(memory_space=pltpu.VMEM)
        held = pl.pallas_call(
            functools.partial(scoped, dims),
            out_shape=(
                pltpu.VMEM((ns // n3 - LATE * SG, kb, jb, ni), BF16),
                pltpu.VMEM((LATE, kj, n1 * rows), BF16),
                pltpu.VMEM((n1 * rows, SG * 2 * ni), BF16),
                pltpu.VMEM(diag_blk.shape, F32),
            ),
            in_specs=[any_space] * 5,
            out_specs=(vmem,) * 4,
            scratch_shapes=scratch,
            compiler_params=pltpu.CompilerParams(collective_id=0, has_side_effects=True, vmem_limit_bytes=50 * 1024 * 1024),
        )(jnp.transpose(vol_blk, (1, 2, 3, 0)), fac_one, fac_two, fac_three, diag_blk)
        return pl.pallas_call(
            finish,
            out_shape=jax.ShapeDtypeStruct((ns // n3, kb, jb, ni), BF16),
            in_specs=[vmem] * 4,
            out_specs=any_space,
            scratch_shapes=[pltpu.VMEM((LATE * SG, kb, jb, ni), BF16), dma((COPIES + LATE,))],
            compiler_params=pltpu.CompilerParams(vmem_limit_bytes=12 * 1024 * 1024),
        )(*held)

    return jax.shard_map(local_step, mesh=mesh, in_specs=(P("dp", "m1", "m2", "m3"), P(), P(), P(), P("m2", "m1", None)), out_specs=P(("dp", "m3"), "m2", "m1", None), check_vma=False)
```

```python
import functools

import jax
import jax.numpy as jnp
from jax import lax
from jax.experimental import pallas as pl
from jax.experimental.pallas import tpu as pltpu
from jax.sharding import PartitionSpec as P

MESH = pl.DeviceIdType.MESH
BF16, F32 = jnp.bfloat16, jnp.float32
SG = 8
SIZES = (2,) * 8
PIECES = len(SIZES)
STARTS = tuple(sum(SIZES[:i]) for i in range(PIECES))
FIRST = (1, 1, 2, 4, 4, 4)
COPIES = 3
LATE = 2
FIRST_SEND_AT = 2
SEND_AT, THIRD_AT = (5, 6), (2, 3)
AHEAD = 2
LANES = 128


def far_first(n):
    return sorted(range(1, n), key=lambda d: -min(d, n - d))


def dot(lhs, rhs, contract=((1,), (0,))):
    return lax.dot_general(lhs, rhs, (contract, ((), ())), preferred_element_type=F32)


def iota(shape, dim):
    return lax.broadcasted_iota(jnp.int32, shape, dim)


def onehot(cond):
    return jnp.where(cond, 1.0, 0.0).astype(BF16)


def third(lhs, w3, d_ref, out, base, shape, pairs=range(SG // 2)):
    ni = shape[-1]
    wide = w3.shape[1] // SG
    scale = d_ref[...].reshape(-1, ni)
    for q in pairs:
        prod = dot(lhs, w3[:, q * 2 * wide : (q + 1) * 2 * wide]).astype(BF16)
        for i in range(2):
            one = prod[:, i * wide : i * wide + ni].astype(F32)
            out[base + 2 * q + i] = (scale * one).astype(BF16).reshape(shape)


def finish(done, last, w3, d_ref, out, tail, sem):
    size = done.shape[0]
    chunk = size // COPIES
    copies = [pltpu.make_async_copy(done.at[pl.ds(i * chunk, chunk)], out.at[pl.ds(i * chunk, chunk)], sem.at[i]) for i in range(COPIES)]
    for c in copies:
        c.start()
    for k in range(LATE):
        third(last[k], w3, d_ref, tail, k * SG, tail.shape[1:])
        copies.append(pltpu.make_async_copy(tail.at[pl.ds(k * SG, SG)], out.at[pl.ds(size + k * SG, SG)], sem.at[COPIES + k]))
        copies[-1].start()
    for c in copies:
        c.wait()


def kernel(dims, x_hbm, a1_hbm, a2_hbm, a3_hbm, d_hbm, out, last, w3, dbuf, xbuf, tbuf, r1, u3, r2, v2, r3, w1, w2, ident, a1, a2, a3,
           in_sem, fac_sem, y_send, y_recv, x_send, x_recv, c_send, c_recv):
    n3, n2, n1, na, nb, nl, ns, nk, nj, ni = dims
    me3, me2, me1 = lax.axis_index("m3"), lax.axis_index("m2"), lax.axis_index("m1")
    groups = ns // n3 // SG
    rows = na * SG
    pairs = na // 2
    kb, jb = nk // n2, nj // n1
    bl, bk, kj = nb * nl, nb * kb, kb * jb
    bt, kt = bl // LANES, bk // LANES
    bs, ks = nb // bt, kb // kt
    half = ks * jb

    loads, cuts = [], [0]
    for n in FIRST:
        part = pl.ds(2 * cuts[-1], 2 * n)
        loads.append(pltpu.make_async_copy(x_hbm.at[part], xbuf.at[part], in_sem.at[len(loads)]))
        cuts.append(cuts[-1] + n)
    facs = [pltpu.make_async_copy(s, t, fac_sem.at[i]) for i, (s, t) in enumerate(((a3_hbm, a3), (a2_hbm, a2), (a1_hbm, a1), (d_hbm, dbuf)))]
    barrier = pltpu.get_barrier_semaphore()
    peers = 0
    other = lax.rem(me1 + 1, n1)
    for axis, me, n, core, first in (("m3", me3, n3, me1, 1), ("m2", me2, n2, other, 0)):
        if axis == "m2":
            loads[0].start()
        for d in range(first, n):
            pl.semaphore_signal(barrier, inc=1, device_id={axis: lax.rem(me + d, n), "m1": core}, device_id_type=MESH)
            peers += 1
    for f in loads[1:] + facs:
        f.start()

    def y_copy(src, dst, sem, d=1):
        return pltpu.make_async_remote_copy(src_ref=src, dst_ref=dst, send_sem=y_send, recv_sem=y_recv.at[sem],
                                            device_id={"m3": lax.rem(me3 + d, n3)}, device_id_type=MESH)

    def x_copy(src, dst, sem, d=1):
        return pltpu.make_async_remote_copy(src_ref=src, dst_ref=dst, send_sem=x_send, recv_sem=x_recv.at[sem],
                                            device_id={"m2": lax.rem(me2 + d, n2), "m1": other}, device_id_type=MESH)

    def c_copy(src, dst, sem):
        return pltpu.make_async_remote_copy(src_ref=src, dst_ref=dst, send_sem=c_send, recv_sem=c_recv.at[sem],
                                            device_id={"m1": other}, device_id_type=MESH)

    def send_pairs(g, lo, n, p):
        at = pl.ds(lo, n)
        for d in far_first(n3):
            y_copy(tbuf.at[d, g, at], r1.at[d - 1, g, at], g * PIECES + p, d).start()

    def send_group(g, part=0, parts=1):
        for p in range(part * PIECES // parts, (part + 1) * PIECES // parts):
            send_pairs(g, STARTS[p], SIZES[p], p)

    sd = ns // n3
    r, c = iota((ns, ns), 0), iota((ns, ns), 1)
    ident[...] = onehot(c == lax.rem(r // sd + me3, n3) * sd + lax.rem(r, sd))

    def build_rest():
        for f in facs[1:]:
            f.wait()
        c = iota((n2 * nb, n2 * LANES), 1)
        pick = onehot(iota((n2 * nb, n2 * LANES), 0) == lax.rem(me2 - c // LANES + n2, n2) * nb + lax.rem(c, LANES) // ks)
        cols2 = dot(a2[...], pick).astype(BF16)
        r, c = iota((half, n2 * LANES), 0), iota((half, n2 * LANES), 1)
        same_k = r // jb == lax.rem(c, ks)
        for e in range(n1):
            r = iota((half, nj), 0)
            sel = onehot(iota((half, nj), 1) == lax.rem(me1 + e, n1) * jb + lax.rem(r, jb))
            w2[e * half : (e + 1) * half, :] = jnp.where(same_k, dot(sel, cols2), 0.0).astype(BF16)

        c = iota((ni, SG * wide), 1)
        pick = onehot(iota((ni, SG * wide), 0) == lax.rem(c, wide))
        cols1 = dot(a1[...], pick, ((0,), (0,))).astype(BF16)
        r, c = iota((rows, SG * wide), 0), iota((rows, SG * wide), 1)
        same_s = lax.rem(r, SG) == c // wide
        for e in range(n1):
            r = iota((rows, n1 * na), 0)
            sel = onehot(iota((rows, n1 * na), 1) == lax.rem(me1 + 1 + e, n1) * na + r // SG)
            w3[e * rows : (e + 1) * rows, :] = jnp.where(same_s, dot(sel, cols1), 0.0).astype(BF16)

    wide = 2 * ni
    eye = ident[...]
    for h, n in enumerate(FIRST):
        loads[h].wait()
        for ap in range(cuts[h], cuts[h + 1]):
            two = [dot(eye, xbuf[2 * ap + i].reshape(bl, ns), ((1,), (1,))).reshape(ns // SG, SG, bl) for i in range(2)]
            tbuf[:, :, ap] = jnp.stack(two, axis=1).reshape(n3, groups, 2 * SG, bl).astype(BF16)
        if h == 0:
            pl.semaphore_wait(barrier, peers)
        for p in range(PIECES):
            lo, hi = max(cuts[h], STARTS[p]), min(cuts[h + 1], STARTS[p] + SIZES[p])
            if lo < hi:
                send_pairs(0, lo, hi - lo, p)

    c = iota((nk, n2 * LANES), 1)
    k_of = lax.rem(c, LANES) // (LANES // kt) * ks + lax.rem(c, ks)
    pick = onehot(iota((nk, n2 * LANES), 0) == lax.rem(c // LANES + me2, n2) * kb + k_of)
    r, c = iota((LANES, n2 * LANES), 0), iota((LANES, n2 * LANES), 1)
    same_b = r // nl == lax.rem(c // ks, bs)
    facs[0].wait()
    cols3 = dot(a3[...], pick, ((0,), (0,))).astype(BF16)
    for d in range(n3):
        r = iota((LANES, n3 * nl), 0)
        sel = onehot(iota((LANES, n3 * nl), 1) == lax.rem(me3 - d + n3, n3) * nl + lax.rem(r, nl))
        w1[d * LANES : (d + 1) * LANES, :] = jnp.where(same_b, dot(sel, cols3), 0.0).astype(BF16)

    def stage1(g, p):
        at, prow = pl.ds(STARTS[p], SIZES[p]), 2 * SG * SIZES[p]
        y_copy(tbuf.at[pl.ds(1, n3 - 1), g, at], r1.at[:, g, at], g * PIECES + p).wait_recv()
        got = [tbuf[0, g, at].reshape(prow, bl)] + [r1[d, g, at].reshape(prow, bl) for d in range(n3 - 1)]
        lhs = [jnp.concatenate([v[:, t * LANES : (t + 1) * LANES] for v in got], axis=1) for t in range(bt)]
        prod = dot(jnp.concatenate(lhs, axis=0), w1[...])
        width = LANES // bt
        slot = iota((prow, LANES), 1) // width
        at = pl.ds(STARTS[p] * 2 * SG, prow)
        for d in range(n2):
            by_b = [prod[t * prow : (t + 1) * prow, d * LANES : (d + 1) * LANES] for t in range(bt)]
            for u in range(kt):
                tile = by_b[u]
                for t in range(bt):
                    if t != u:
                        tile = jnp.where(slot == t, pltpu.roll(by_b[t], (t - u) * width % LANES, 1), tile)
                u3[d, g, at, u * LANES : (u + 1) * LANES] = tile.astype(BF16)
        for d in (*far_first(n2), 0):
            x_copy(u3.at[d, g, at], r2.at[d, g, at], 2 * g + 2 * STARTS[p] // pairs, d).start()

    def x_wait(g, part):
        at = pl.ds(part * rows // 2, rows // 2)
        x_copy(u3.at[:, g, at], r2.at[:, g, at], 2 * g + part).wait_recv()

    def second(g, u, es, col=slice(None), send=True):
        got = [r2.at[d, g, col] for d in range(n2)]
        rhs = jnp.concatenate([v[:, u * LANES : (u + 1) * LANES] for v in got], axis=1)
        prod = dot(w2[es[0] * half : (es[-1] + 1) * half, :], rhs, ((1,), (1,))).astype(BF16)
        at = pl.ds(u * half, half)
        for k, e in enumerate(es):
            v2[e, g, at, col] = prod[k * half : (k + 1) * half, :]
        if 1 in es and send:
            c_copy(v2.at[1, g, at, col], r3.at[g, at, col], g).start()

    def stage2(g, u):
        if u == 0:
            for part in range(2):
                x_wait(g, part)
        second(g, u, tuple(range(n1)))

    def stage3(g, part=0, parts=1):
        if part == 0:
            c_copy(v2.at[1, g], r3.at[g], g).wait_recv()
        third(jnp.concatenate([v2[0, g], r3[g]], axis=1), w3, dbuf, out, g * SG, (kb, jb, ni), range(part * SG // 2 // parts, (part + 1) * SG // 2 // parts))

    def step(g, carry):
        def later(p, lag, act):
            pl.when(g >= lag)(lambda: act(g - lag))

        for p in range(PIECES):
            stage1(g, p)
            if p == 0:
                later(p, 2, lambda k: stage2(k, 1))
            if p == FIRST_SEND_AT:
                for k in range(1, AHEAD):
                    pl.when(g == 0)(functools.partial(send_group, k))
            if p in SEND_AT:
                pl.when(g + AHEAD < groups)(lambda: send_group(g + AHEAD, SEND_AT.index(p), len(SEND_AT)))
            if p in THIRD_AT:
                later(p, 3, lambda k: stage3(k, THIRD_AT.index(p), len(THIRD_AT)))
        pl.when(g == 0)(build_rest)
        later(p, 1, lambda k: stage2(k, 0))
        return carry

    lax.fori_loop(0, groups, step, 0)
    fin = groups - 1
    stage2(fin - 1, 1)
    stage3(fin - 2)
    def hand_over(g):
        c_copy(v2.at[1, g], r3.at[g], g).wait_recv()
        last[g - groups + LATE, :, :rows] = v2[0, g]
        last[g - groups + LATE, :, rows:] = r3[g]

    for part in range(2):
        x_wait(fin, part)
        col = pl.ds(part * rows // 2, rows // 2)
        for u in range(kt):
            second(fin, u, (1,), col, False)
        c_copy(v2.at[1, fin, :, col], r3.at[fin, :, col], fin).start()
        if part == 0:
            hand_over(fin - 1)
    for u in range(kt):
        second(fin, u, (0,))
    hand_over(fin)

    y_copy(tbuf.at[pl.ds(1, n3 - 1)], r1, 0).wait_send()
    x_copy(u3, r2, 0).wait_send()
    c_copy(v2.at[1], r3, 0).wait_send()


def scoped(dims, *refs):
    dma = pltpu.SemaphoreType.DMA
    n3, ns = dims[0], dims[6]
    groups = ns // n3 // SG
    pl.run_scoped(functools.partial(kernel, dims, *refs), dma((len(FIRST),)), dma((4,)), dma, dma((groups * PIECES,)), dma, dma((2 * groups,)), dma, dma((groups,)))


def solution(mesh):
    n3, n2, n1 = mesh.shape["m3"], mesh.shape["m2"], mesh.shape["m1"]

    def local_step(vol_blk, fac_one, fac_two, fac_three, diag_blk):
        ns, na, nb, nl = vol_blk.shape
        nk, nj, ni = fac_three.shape[0], fac_two.shape[0], fac_one.shape[0]
        kb, jb = nk // n2, nj // n1
        groups, rows = ns // n3 // SG, na * SG
        bl, bk, kj = nb * nl, nb * kb, kb * jb
        dims = (n3, n2, n1, na, nb, nl, ns, nk, nj, ni)
        dma = pltpu.SemaphoreType.DMA
        any_space = pl.BlockSpec(memory_space=pl.ANY)
        scratch = [
            pltpu.VMEM((na, nb, nl, ns), BF16),
            pltpu.VMEM((n3, groups, na // 2, 2 * SG, bl), BF16),
            pltpu.VMEM((n3 - 1, groups, na // 2, 2 * SG, bl), BF16),
            pltpu.VMEM((n2, groups, rows, bk), BF16),
            pltpu.VMEM((n2, groups, rows, bk), BF16),
            pltpu.VMEM((n1, groups, kj, rows), BF16),
            pltpu.VMEM((groups, kj, rows), BF16),
            pltpu.VMEM((n3 * LANES, n2 * LANES), BF16),
            pltpu.VMEM((n1 * kj * LANES // bk, n2 * LANES), BF16),
            pltpu.VMEM((ns, ns), BF16),
            pltpu.VMEM(fac_one.shape, BF16),
            pltpu.VMEM(fac_two.shape, BF16),
            pltpu.VMEM(fac_three.shape, BF16),
        ]
        vmem = pl.BlockSpec(memory_space=pltpu.VMEM)
        held = pl.pallas_call(
            functools.partial(scoped, dims),
            out_shape=(
                pltpu.VMEM((ns // n3 - LATE * SG, kb, jb, ni), BF16),
                pltpu.VMEM((LATE, kj, n1 * rows), BF16),
                pltpu.VMEM((n1 * rows, SG * 2 * ni), BF16),
                pltpu.VMEM(diag_blk.shape, F32),
            ),
            in_specs=[any_space] * 5,
            out_specs=(vmem,) * 4,
            scratch_shapes=scratch,
            compiler_params=pltpu.CompilerParams(collective_id=0, has_side_effects=True, vmem_limit_bytes=50 * 1024 * 1024),
        )(jnp.transpose(vol_blk, (1, 2, 3, 0)), fac_one, fac_two, fac_three, diag_blk)
        return pl.pallas_call(
            finish,
            out_shape=jax.ShapeDtypeStruct((ns // n3, kb, jb, ni), BF16),
            in_specs=[vmem] * 4,
            out_specs=any_space,
            scratch_shapes=[pltpu.VMEM((LATE * SG, kb, jb, ni), BF16), dma((COPIES + LATE,))],
            compiler_params=pltpu.CompilerParams(vmem_limit_bytes=12 * 1024 * 1024),
        )(*held)

    return jax.shard_map(local_step, mesh=mesh, in_specs=(P("dp", "m1", "m2", "m3"), P(), P(), P(), P("m2", "m1", None)), out_specs=P(("dp", "m3"), "m2", "m1", None), check_vma=False)
```

```python
import functools

import jax
import jax.numpy as jnp
from jax import lax
from jax.experimental import pallas as pl
from jax.experimental.pallas import tpu as pltpu
from jax.sharding import PartitionSpec as P

MESH = pl.DeviceIdType.MESH
BF16, F32 = jnp.bfloat16, jnp.float32
SG = 8
SIZES = (2,) * 8
PIECES = len(SIZES)
STARTS = tuple(sum(SIZES[:i]) for i in range(PIECES))
FIRST = (1, 1, 1, 1, 4, 8)
COPIES = 3
LATE = 2
FIRST_SEND_AT = 2
SEND_AT, THIRD_AT = (5, 6), (2, 3)
AHEAD = 2
LANES = 128


def far_first(n):
    return sorted(range(1, n), key=lambda d: -min(d, n - d))


def dot(lhs, rhs, contract=((1,), (0,))):
    return lax.dot_general(lhs, rhs, (contract, ((), ())), preferred_element_type=F32)


def iota(shape, dim):
    return lax.broadcasted_iota(jnp.int32, shape, dim)


def onehot(cond):
    return jnp.where(cond, 1.0, 0.0).astype(BF16)


def third(lhs, w3, d_ref, out, base, shape, pairs=range(SG // 2)):
    ni = shape[-1]
    wide = w3.shape[1] // SG
    scale = d_ref[...].reshape(-1, ni)
    for q in pairs:
        prod = dot(lhs, w3[:, q * 2 * wide : (q + 1) * 2 * wide]).astype(BF16)
        for i in range(2):
            one = prod[:, i * wide : i * wide + ni].astype(F32)
            out[base + 2 * q + i] = (scale * one).astype(BF16).reshape(shape)


def finish(done, last, w3, d_ref, out, tail, sem):
    size = done.shape[0]
    chunk = size // COPIES
    copies = [pltpu.make_async_copy(done.at[pl.ds(i * chunk, chunk)], out.at[pl.ds(i * chunk, chunk)], sem.at[i]) for i in range(COPIES)]
    for c in copies:
        c.start()
    for k in range(LATE):
        third(last[k], w3, d_ref, tail, k * SG, tail.shape[1:])
        copies.append(pltpu.make_async_copy(tail.at[pl.ds(k * SG, SG)], out.at[pl.ds(size + k * SG, SG)], sem.at[COPIES + k]))
        copies[-1].start()
    for c in copies:
        c.wait()


def kernel(dims, x_hbm, a1_hbm, a2_hbm, a3_hbm, d_hbm, out, last, w3, dbuf, xbuf, tbuf, r1, u3, r2, v2, r3, w1, w2, ident, a1, a2, a3,
           in_sem, fac_sem, y_send, y_recv, x_send, x_recv, c_send, c_recv):
    n3, n2, n1, na, nb, nl, ns, nk, nj, ni = dims
    me3, me2, me1 = lax.axis_index("m3"), lax.axis_index("m2"), lax.axis_index("m1")
    groups = ns // n3 // SG
    rows = na * SG
    pairs = na // 2
    kb, jb = nk // n2, nj // n1
    bl, bk, kj = nb * nl, nb * kb, kb * jb
    bt, kt = bl // LANES, bk // LANES
    bs, ks = nb // bt, kb // kt
    half = ks * jb

    loads, cuts = [], [0]
    for n in FIRST:
        part = pl.ds(2 * cuts[-1], 2 * n)
        loads.append(pltpu.make_async_copy(x_hbm.at[part], xbuf.at[part], in_sem.at[len(loads)]))
        cuts.append(cuts[-1] + n)
    facs = [pltpu.make_async_copy(s, t, fac_sem.at[i]) for i, (s, t) in enumerate(((a3_hbm, a3), (a2_hbm, a2), (a1_hbm, a1), (d_hbm, dbuf)))]
    barrier = pltpu.get_barrier_semaphore()
    peers = 0
    other = lax.rem(me1 + 1, n1)
    for axis, me, n, core, first in (("m3", me3, n3, me1, 1), ("m2", me2, n2, other, 0)):
        if axis == "m2":
            loads[0].start()
        for d in range(first, n):
            pl.semaphore_signal(barrier, inc=1, device_id={axis: lax.rem(me + d, n), "m1": core}, device_id_type=MESH)
            peers += 1
    for f in loads[1:] + facs:
        f.start()

    def y_copy(src, dst, sem, d=1):
        return pltpu.make_async_remote_copy(src_ref=src, dst_ref=dst, send_sem=y_send, recv_sem=y_recv.at[sem],
                                            device_id={"m3": lax.rem(me3 + d, n3)}, device_id_type=MESH)

    def x_copy(src, dst, sem, d=1):
        return pltpu.make_async_remote_copy(src_ref=src, dst_ref=dst, send_sem=x_send, recv_sem=x_recv.at[sem],
                                            device_id={"m2": lax.rem(me2 + d, n2), "m1": other}, device_id_type=MESH)

    def c_copy(src, dst, sem):
        return pltpu.make_async_remote_copy(src_ref=src, dst_ref=dst, send_sem=c_send, recv_sem=c_recv.at[sem],
                                            device_id={"m1": other}, device_id_type=MESH)

    def send_pairs(g, lo, n, p):
        at = pl.ds(lo, n)
        for d in far_first(n3):
            y_copy(tbuf.at[d, g, at], r1.at[d - 1, g, at], g * PIECES + p, d).start()

    def send_group(g, part=0, parts=1):
        for p in range(part * PIECES // parts, (part + 1) * PIECES // parts):
            send_pairs(g, STARTS[p], SIZES[p], p)

    sd = ns // n3
    r, c = iota((ns, ns), 0), iota((ns, ns), 1)
    ident[...] = onehot(c == lax.rem(r // sd + me3, n3) * sd + lax.rem(r, sd))

    def build_rest():
        for f in facs[1:]:
            f.wait()
        c = iota((n2 * nb, n2 * LANES), 1)
        pick = onehot(iota((n2 * nb, n2 * LANES), 0) == lax.rem(me2 - c // LANES + n2, n2) * nb + lax.rem(c, LANES) // ks)
        cols2 = dot(a2[...], pick).astype(BF16)
        r, c = iota((half, n2 * LANES), 0), iota((half, n2 * LANES), 1)
        same_k = r // jb == lax.rem(c, ks)
        for e in range(n1):
            r = iota((half, nj), 0)
            sel = onehot(iota((half, nj), 1) == lax.rem(me1 + e, n1) * jb + lax.rem(r, jb))
            w2[e * half : (e + 1) * half, :] = jnp.where(same_k, dot(sel, cols2), 0.0).astype(BF16)

        c = iota((ni, SG * wide), 1)
        pick = onehot(iota((ni, SG * wide), 0) == lax.rem(c, wide))
        cols1 = dot(a1[...], pick, ((0,), (0,))).astype(BF16)
        r, c = iota((rows, SG * wide), 0), iota((rows, SG * wide), 1)
        same_s = lax.rem(r, SG) == c // wide
        for e in range(n1):
            r = iota((rows, n1 * na), 0)
            sel = onehot(iota((rows, n1 * na), 1) == lax.rem(me1 + 1 + e, n1) * na + r // SG)
            w3[e * rows : (e + 1) * rows, :] = jnp.where(same_s, dot(sel, cols1), 0.0).astype(BF16)

    wide = 2 * ni
    eye = ident[...]
    for h, n in enumerate(FIRST):
        loads[h].wait()
        for ap in range(cuts[h], cuts[h + 1]):
            two = [dot(eye, xbuf[2 * ap + i].reshape(bl, ns), ((1,), (1,))).reshape(ns // SG, SG, bl) for i in range(2)]
            tbuf[:, :, ap] = jnp.stack(two, axis=1).reshape(n3, groups, 2 * SG, bl).astype(BF16)
        if h == 0:
            pl.semaphore_wait(barrier, peers)
        for p in range(PIECES):
            lo, hi = max(cuts[h], STARTS[p]), min(cuts[h + 1], STARTS[p] + SIZES[p])
            if lo < hi:
                send_pairs(0, lo, hi - lo, p)

    c = iota((nk, n2 * LANES), 1)
    k_of = lax.rem(c, LANES) // (LANES // kt) * ks + lax.rem(c, ks)
    pick = onehot(iota((nk, n2 * LANES), 0) == lax.rem(c // LANES + me2, n2) * kb + k_of)
    r, c = iota((LANES, n2 * LANES), 0), iota((LANES, n2 * LANES), 1)
    same_b = r // nl == lax.rem(c // ks, bs)
    facs[0].wait()
    cols3 = dot(a3[...], pick, ((0,), (0,))).astype(BF16)
    for d in range(n3):
        r = iota((LANES, n3 * nl), 0)
        sel = onehot(iota((LANES, n3 * nl), 1) == lax.rem(me3 - d + n3, n3) * nl + lax.rem(r, nl))
        w1[d * LANES : (d + 1) * LANES, :] = jnp.where(same_b, dot(sel, cols3), 0.0).astype(BF16)

    def stage1(g, p):
        at, prow = pl.ds(STARTS[p], SIZES[p]), 2 * SG * SIZES[p]
        y_copy(tbuf.at[pl.ds(1, n3 - 1), g, at], r1.at[:, g, at], g * PIECES + p).wait_recv()
        got = [tbuf[0, g, at].reshape(prow, bl)] + [r1[d, g, at].reshape(prow, bl) for d in range(n3 - 1)]
        lhs = [jnp.concatenate([v[:, t * LANES : (t + 1) * LANES] for v in got], axis=1) for t in range(bt)]
        prod = dot(jnp.concatenate(lhs, axis=0), w1[...])
        width = LANES // bt
        slot = iota((prow, LANES), 1) // width
        at = pl.ds(STARTS[p] * 2 * SG, prow)
        for d in range(n2):
            by_b = [prod[t * prow : (t + 1) * prow, d * LANES : (d + 1) * LANES] for t in range(bt)]
            for u in range(kt):
                tile = by_b[u]
                for t in range(bt):
                    if t != u:
                        tile = jnp.where(slot == t, pltpu.roll(by_b[t], (t - u) * width % LANES, 1), tile)
                u3[d, g, at, u * LANES : (u + 1) * LANES] = tile.astype(BF16)
        for d in (*far_first(n2), 0):
            x_copy(u3.at[d, g, at], r2.at[d, g, at], 2 * g + 2 * STARTS[p] // pairs, d).start()

    def x_wait(g, part):
        at = pl.ds(part * rows // 2, rows // 2)
        x_copy(u3.at[:, g, at], r2.at[:, g, at], 2 * g + part).wait_recv()

    def second(g, u, es, col=slice(None), send=True):
        got = [r2.at[d, g, col] for d in range(n2)]
        rhs = jnp.concatenate([v[:, u * LANES : (u + 1) * LANES] for v in got], axis=1)
        prod = dot(w2[es[0] * half : (es[-1] + 1) * half, :], rhs, ((1,), (1,))).astype(BF16)
        at = pl.ds(u * half, half)
        for k, e in enumerate(es):
            v2[e, g, at, col] = prod[k * half : (k + 1) * half, :]
        if 1 in es and send:
            c_copy(v2.at[1, g, at, col], r3.at[g, at, col], g).start()

    def stage2(g, u):
        if u == 0:
            for part in range(2):
                x_wait(g, part)
        second(g, u, tuple(range(n1)))

    def stage3(g, part=0, parts=1):
        if part == 0:
            c_copy(v2.at[1, g], r3.at[g], g).wait_recv()
        third(jnp.concatenate([v2[0, g], r3[g]], axis=1), w3, dbuf, out, g * SG, (kb, jb, ni), range(part * SG // 2 // parts, (part + 1) * SG // 2 // parts))

    def step(g, carry):
        def later(p, lag, act):
            pl.when(g >= lag)(lambda: act(g - lag))

        for p in range(PIECES):
            stage1(g, p)
            if p == 0:
                later(p, 2, lambda k: stage2(k, 1))
            if p == FIRST_SEND_AT:
                for k in range(1, AHEAD):
                    pl.when(g == 0)(functools.partial(send_group, k))
            if p in SEND_AT:
                pl.when(g + AHEAD < groups)(lambda: send_group(g + AHEAD, SEND_AT.index(p), len(SEND_AT)))
            if p in THIRD_AT:
                later(p, 3, lambda k: stage3(k, THIRD_AT.index(p), len(THIRD_AT)))
        pl.when(g == 0)(build_rest)
        later(p, 1, lambda k: stage2(k, 0))
        return carry

    lax.fori_loop(0, groups, step, 0)
    fin = groups - 1
    stage2(fin - 1, 1)
    stage3(fin - 2)
    def hand_over(g):
        c_copy(v2.at[1, g], r3.at[g], g).wait_recv()
        last[g - groups + LATE, :, :rows] = v2[0, g]
        last[g - groups + LATE, :, rows:] = r3[g]

    for part in range(2):
        x_wait(fin, part)
        col = pl.ds(part * rows // 2, rows // 2)
        for u in range(kt):
            second(fin, u, (1,), col, False)
        c_copy(v2.at[1, fin, :, col], r3.at[fin, :, col], fin).start()
        if part == 0:
            hand_over(fin - 1)
    for u in range(kt):
        second(fin, u, (0,))
    hand_over(fin)

    y_copy(tbuf.at[pl.ds(1, n3 - 1)], r1, 0).wait_send()
    x_copy(u3, r2, 0).wait_send()
    c_copy(v2.at[1], r3, 0).wait_send()


def scoped(dims, *refs):
    dma = pltpu.SemaphoreType.DMA
    n3, ns = dims[0], dims[6]
    groups = ns // n3 // SG
    pl.run_scoped(functools.partial(kernel, dims, *refs), dma((len(FIRST),)), dma((4,)), dma, dma((groups * PIECES,)), dma, dma((2 * groups,)), dma, dma((groups,)))


def solution(mesh):
    n3, n2, n1 = mesh.shape["m3"], mesh.shape["m2"], mesh.shape["m1"]

    def local_step(vol_blk, fac_one, fac_two, fac_three, diag_blk):
        ns, na, nb, nl = vol_blk.shape
        nk, nj, ni = fac_three.shape[0], fac_two.shape[0], fac_one.shape[0]
        kb, jb = nk // n2, nj // n1
        groups, rows = ns // n3 // SG, na * SG
        bl, bk, kj = nb * nl, nb * kb, kb * jb
        dims = (n3, n2, n1, na, nb, nl, ns, nk, nj, ni)
        dma = pltpu.SemaphoreType.DMA
        any_space = pl.BlockSpec(memory_space=pl.ANY)
        scratch = [
            pltpu.VMEM((na, nb, nl, ns), BF16),
            pltpu.VMEM((n3, groups, na // 2, 2 * SG, bl), BF16),
            pltpu.VMEM((n3 - 1, groups, na // 2, 2 * SG, bl), BF16),
            pltpu.VMEM((n2, groups, rows, bk), BF16),
            pltpu.VMEM((n2, groups, rows, bk), BF16),
            pltpu.VMEM((n1, groups, kj, rows), BF16),
            pltpu.VMEM((groups, kj, rows), BF16),
            pltpu.VMEM((n3 * LANES, n2 * LANES), BF16),
            pltpu.VMEM((n1 * kj * LANES // bk, n2 * LANES), BF16),
            pltpu.VMEM((ns, ns), BF16),
            pltpu.VMEM(fac_one.shape, BF16),
            pltpu.VMEM(fac_two.shape, BF16),
            pltpu.VMEM(fac_three.shape, BF16),
        ]
        vmem = pl.BlockSpec(memory_space=pltpu.VMEM)
        held = pl.pallas_call(
            functools.partial(scoped, dims),
            out_shape=(
                pltpu.VMEM((ns // n3 - LATE * SG, kb, jb, ni), BF16),
                pltpu.VMEM((LATE, kj, n1 * rows), BF16),
                pltpu.VMEM((n1 * rows, SG * 2 * ni), BF16),
                pltpu.VMEM(diag_blk.shape, F32),
            ),
            in_specs=[any_space] * 5,
            out_specs=(vmem,) * 4,
            scratch_shapes=scratch,
            compiler_params=pltpu.CompilerParams(collective_id=0, has_side_effects=True, vmem_limit_bytes=50 * 1024 * 1024),
        )(jnp.transpose(vol_blk, (1, 2, 3, 0)), fac_one, fac_two, fac_three, diag_blk)
        return pl.pallas_call(
            finish,
            out_shape=jax.ShapeDtypeStruct((ns // n3, kb, jb, ni), BF16),
            in_specs=[vmem] * 4,
            out_specs=any_space,
            scratch_shapes=[pltpu.VMEM((LATE * SG, kb, jb, ni), BF16), dma((COPIES + LATE,))],
            compiler_params=pltpu.CompilerParams(vmem_limit_bytes=12 * 1024 * 1024),
        )(*held)

    return jax.shard_map(local_step, mesh=mesh, in_specs=(P("dp", "m1", "m2", "m3"), P(), P(), P(), P("m2", "m1", None)), out_specs=P(("dp", "m3"), "m2", "m1", None), check_vma=False)
```
